256 devices in a mesh: dp: 16 (over z, core), sx: 4 (over y), sy: 4 (over x).
Axes of the slice: x: 4, y: 4, z: 8, core: 2. Of those that a mesh axis runs over, the one named last changes fastest.
Arguments:
- volume: bfloat16 [16, 32, 32, 32, 128], P('dp', None, 'sx', 'sy'), may hold values from -6 to 6
- conv_one: bfloat16 [16, 32, 32, 32, 128], P('dp', None, 'sx', 'sy'), may hold values from -300 to 300
- conv_two: bfloat16 [16, 32, 32, 32, 128], P('dp', None, 'sx', 'sy'), may hold values from -300 to 300
- upper_grad: bfloat16 [16, 32, 32, 32, 128], P('dp', None, 'sx', 'sy'), may hold values from -36 to 36
- weight_one: bfloat16 [3, 3, 3, 32, 32], replicated, may hold values from -0.21875 to 0.21875
- weight_two: bfloat16 [3, 3, 3, 32, 32], replicated, may hold values from -0.21875 to 0.21875
- gain_one: float32 [32], replicated, may hold values from 0.1 to 1.9
- bias_one: float32 [32], replicated, may hold values from -1 to 1
- gain_two: float32 [32], replicated, may hold values from 0.1 to 1.9
- bias_two: float32 [32], replicated, may hold values from -1 to 1
Outputs:
- input_grad: bfloat16 [16, 32, 32, 32, 128], P('dp', None, 'sx', 'sy')
- weight_one_grad: float32 [3, 3, 3, 32, 32], replicated
- weight_two_grad: float32 [3, 3, 3, 32, 32], replicated
- gain_one_grad: float32 [32], replicated
- bias_one_grad: float32 [32], replicated
- gain_two_grad: float32 [32], replicated
- bias_two_grad: float32 [32], replicated
The draws below stay inside these ranges and needn't reach their ends.
All inputs are finite; a program needn't handle non-finite values.
Results may differ from the reference program's by a relative error of at most 0.014.
Values may be sent and summed in bfloat16 or wider, within the bound.
No kernel may reach another device: no remote copies, remote signals or barrier semaphores. Data moves between devices by JAX's collectives and lax.ppermute only.
A program may use at most 64 MiB of HBM per device.

```python
import math
import jax
import jax.numpy as jnp
from jax import lax

C = 32
CZ = 128
VOLS = 16
NX = 32
NY = 32


def rising_scale():
    volumes = jnp.arange(VOLS, dtype=jnp.float32) / max(VOLS - 1, 1)
    across = jnp.arange(NX, dtype=jnp.float32) / max(NX - 1, 1)
    along = jnp.arange(NY, dtype=jnp.float32) / max(NY - 1, 1)
    exponent = volumes[:, None, None, None, None] + across[None, None, :, None, None] + along[None, None, None, :, None] - 1.5
    return jnp.exp(exponent * math.log(3.0))


def saved_field(key):
    first, second, third = jax.random.split(key, 3)
    shape = (VOLS, C, NX, NY, CZ)
    offset = jax.random.uniform(first, (1, C, 1, 1, 1), jnp.float32, -1.0, 1.0)
    noise = jax.random.truncated_normal(second, -4.0, 4.0, shape, jnp.float32)
    factor = jnp.exp(jax.random.uniform(third, (VOLS, 1, NX, NY, CZ), jnp.float32, 0.0, math.log(10.0)))
    values = (offset + noise) * factor
    return (values * rising_scale()).astype(jnp.bfloat16)


def draw_conv_one(key, part):
    return saved_field(jax.random.fold_in(key, 11))


def draw_conv_two(key, part):
    return saved_field(jax.random.fold_in(key, 12))


def draw_upper_grad(key, part):
    first = jax.random.fold_in(jax.random.fold_in(key, 13), 0)
    shape = (VOLS, C, NX, NY, CZ)
    values = jax.random.truncated_normal(first, -4.0, 4.0, shape, jnp.float32)
    return (values * rising_scale()).astype(jnp.bfloat16)


def steps_of(own_key, extent, cuts, low, high):
    level = 1.0
    for axis_at, parts in cuts:
        steps = jax.random.uniform(jax.random.fold_in(jax.random.fold_in(own_key, 6), axis_at), (parts,), jnp.float32, low / len(cuts), high / len(cuts))
        level = level * jnp.repeat(jnp.exp(steps), extent[axis_at] // parts).reshape((-1,) + (1,) * (len(extent) - 1 - axis_at))
    return level


def scatter_about(stream_key, dims, deviation, bound, cuts=(), kind=jnp.bfloat16):
    array = jax.random.normal(stream_key, dims, jnp.float32) * deviation
    if len(cuts) > 0:
        array = steps_of(stream_key, dims, cuts, -0.22, 0.18) * array
    return jnp.clip(array, min=-bound, max=bound).astype(kind)


def setup_inputs(seed: int = 0) -> dict:
    key_of = jax.random.split(jax.random.key(seed), 11)
    volume = scatter_about(key_of[0], (VOLS, C, NX, NY, CZ), 1.0, 6.0, ((0, 16), (2, 4), (3, 4)))
    conv_one = draw_conv_one(jax.random.fold_in(key_of[10], 71), 0)
    conv_two = draw_conv_two(jax.random.fold_in(key_of[10], 71), 0)
    upper_grad = draw_upper_grad(jax.random.fold_in(key_of[10], 71), 0)
    weight_one = scatter_about(key_of[4], (3, 3, 3, C, C), (27 * C) ** -0.5, 0.21875)
    weight_two = scatter_about(key_of[5], (3, 3, 3, C, C), (27 * C) ** -0.5, 0.21875)
    gain_one = jnp.clip(1.0 + 0.18 * jax.random.normal(key_of[6], (C,), jnp.float32), 0.1, 1.9)
    bias_one = jnp.clip(jax.random.uniform(key_of[7], (C,), jnp.float32, -1.0, 1.0), -1.0, 1.0)
    gain_two = jnp.clip(1.0 + 0.18 * jax.random.normal(key_of[8], (C,), jnp.float32), 0.1, 1.9)
    bias_two = jnp.clip(jax.random.uniform(key_of[9], (C,), jnp.float32, -1.0, 1.0), -1.0, 1.0)
    return {"volume": volume, "conv_one": conv_one, "conv_two": conv_two, "upper_grad": upper_grad, "weight_one": weight_one, "weight_two": weight_two, "gain_one": gain_one, "bias_one": bias_one, "gain_two": gain_two, "bias_two": bias_two}


epsilon = 1e-05

def channel(vector):
    return vector[None, :, None, None, None]

def pad_space(values):
    return jnp.pad(values.astype(jnp.float32), ((0, 0), (0, 0), (1, 1), (1, 1), (1, 1)))

def back_project(gradient, weight):
    padded = pad_space(gradient)
    extent_x, extent_y, extent_z = (gradient.shape[2], gradient.shape[3], gradient.shape[4])
    total = jnp.zeros(gradient.shape, jnp.float32)
    for shift_x in range(3):
        for shift_y in range(3):
            for shift_z in range(3):
                piece = padded[:, :, 2 - shift_x:2 - shift_x + extent_x, 2 - shift_y:2 - shift_y + extent_y, 2 - shift_z:2 - shift_z + extent_z]
                total = total + jnp.einsum('co,boxyz->bcxyz', weight[shift_x, shift_y, shift_z].astype(jnp.float32), piece, precision=lax.Precision.HIGHEST)
    return total

def filter_terms(values, gradient):
    padded = pad_space(values)
    grad_full = gradient.astype(jnp.float32)
    extent_x, extent_y, extent_z = (gradient.shape[2], gradient.shape[3], gradient.shape[4])
    blocks = []
    for shift_x in range(3):
        for shift_y in range(3):
            for shift_z in range(3):
                piece = padded[:, :, shift_x:shift_x + extent_x, shift_y:shift_y + extent_y, shift_z:shift_z + extent_z]
                blocks.append(jnp.einsum('bcxyz,boxyz->co', piece, grad_full, precision=lax.Precision.HIGHEST))
    width = values.shape[1]
    return jnp.stack(blocks).reshape(3, 3, 3, width, gradient.shape[1])

def silu_slope(inputs):
    logistic = jax.nn.sigmoid(inputs)
    return logistic * (1.0 + inputs * (1.0 - logistic))

def normalized(saved, gain, offset, cell_count):
    saved_full = saved.astype(jnp.float32)
    total = lax.optimization_barrier(jnp.sum(saved_full, axis=(0, 2, 3, 4)))
    squares = lax.optimization_barrier(jnp.sum(saved_full * saved_full, axis=(0, 2, 3, 4)))
    average = total / cell_count
    spread = squares / cell_count - average * average
    inv_std = lax.rsqrt(spread + epsilon)
    centered = (saved_full - channel(average)) * channel(inv_std)
    shifted = channel(gain) * centered + channel(offset)
    return (centered, shifted, inv_std)

def norm_backward(upstream, centered, shifted, inv_std, gain, cell_count):
    slope_grad = upstream * silu_slope(shifted)
    bias_total = lax.optimization_barrier(jnp.sum(slope_grad, axis=(0, 2, 3, 4)))
    gain_total = lax.optimization_barrier(jnp.sum(slope_grad * centered, axis=(0, 2, 3, 4)))
    pre_grad = channel(gain * inv_std) * (slope_grad - channel(bias_total / cell_count) - centered * channel(gain_total / cell_count))
    return (pre_grad.astype(jnp.bfloat16), gain_total, bias_total)

def reference(volume, conv_one, conv_two, upper_grad, weight_one, weight_two, gain_one, bias_one, gain_two, bias_two):
    cell_count = float(VOLS * NX * NY * CZ)
    cent_one, shift_one, inv_one = normalized(conv_one, gain_one, bias_one, cell_count)
    activation = jax.nn.silu(shift_one).astype(jnp.bfloat16)
    cent_two, shift_two, inv_two = normalized(conv_two, gain_two, bias_two, cell_count)
    grad_two, gain_two_total, bias_two_total = norm_backward(upper_grad.astype(jnp.float32), cent_two, shift_two, inv_two, gain_two, cell_count)
    upstream = back_project(grad_two, weight_two)
    filter_two = filter_terms(activation, grad_two)
    grad_one, gain_one_total, bias_one_total = norm_backward(upstream, cent_one, shift_one, inv_one, gain_one, cell_count)
    input_grad = back_project(grad_one, weight_one).astype(jnp.bfloat16)
    filter_one = filter_terms(volume, grad_one)
    factor = 1.0 / math.sqrt(cell_count)
    return (input_grad, filter_one * factor, filter_two * factor, gain_one_total * factor, bias_one_total * factor, gain_two_total * factor, bias_two_total * factor)
```

```python
import functools
import math

import jax
import jax.numpy as jnp
from jax import lax
from jax.experimental import pallas as pl
from jax.experimental.pallas import tpu as pltpu
from jax.sharding import Mesh
from jax.sharding import PartitionSpec as P

DP = ("dp_0", "dp_1")
ALL = ("dp_0", "dp_1", "sx", "sy")
PLANE = ("dp_1", "sx", "sy")
EPS = 1e-05
F32 = jnp.float32
BF16 = jnp.bfloat16
C = 32
B = 8
Z = 128
CELLS = float(16 * 32 * 32 * Z)
SCALE = 1.0 / math.sqrt(CELLS)

SIDES = tuple((dx, dy) for dx in (-1, 0, 1) for dy in (-1, 0, 1) if (dx, dy) != (0, 0))
VMEM = pltpu.MemorySpace.VMEM
SMEM = pltpu.MemorySpace.SMEM


def span(d, width):
    if d == 0:
        return range(B)
    return range(B - width, B) if d > 0 else range(width)


def landing(d, width):
    if d == 0:
        return range(width, B + width)
    return range(B + width, B + 2 * width) if d > 0 else range(width)


def slabs(side):
    out = []
    for which, width in (("c2", 2), ("ug", 2), ("c1", 1)):
        for x in span(side[0], width):
            for y in span(side[1], width):
                out.append((which, x, y))
    return out


def places(side):
    out = []
    for which, width in (("c2", 2), ("ug", 2), ("c1", 1)):
        for x in landing(side[0], width):
            for y in landing(side[1], width):
                out.append((which, x, y))
    return out


def call(kernel, outs, scratch=(), flops=0, n_smem=0, n_in=0):
    single = not isinstance(outs, (list, tuple))
    shapes = [outs] if single else list(outs)
    f = pl.pallas_call(
        kernel,
        out_shape=shapes[0] if single else tuple(shapes),
        in_specs=[pl.BlockSpec(memory_space=SMEM)] * n_smem
        + [pl.BlockSpec(memory_space=VMEM)] * (n_in - n_smem),
        out_specs=pl.BlockSpec(memory_space=VMEM)
        if single
        else tuple(pl.BlockSpec(memory_space=VMEM) for _ in shapes),
        scratch_shapes=list(scratch),
        compiler_params=pltpu.CompilerParams(vmem_limit_bytes=40 * 2**20),
        cost_estimate=pl.CostEstimate(flops=flops, bytes_accessed=1 << 20, transcendentals=0),
    )
    return f


def shaped(dims, kind):
    return jax.ShapeDtypeStruct(dims, kind)


def across(columns):
    return jnp.sum(jnp.transpose(columns), axis=0, keepdims=True)


def down(row):
    return jnp.transpose(jnp.broadcast_to(row, (128, 128)))


def arrived(ref):
    total = jnp.sum(ref[...].reshape(ref.shape[0], 128), axis=0, keepdims=True)
    return total


def stats_kernel(one_ref, two_ref, out_ref):
    parts = []
    for ref in (one_ref, two_ref):
        sums, squares = [], []
        for c in range(C):
            block = ref[0, c].astype(F32)
            sums.append(jnp.sum(jnp.sum(block, axis=0), axis=0, keepdims=True))
            squares.append(jnp.sum(jnp.sum(block * block, axis=0), axis=0, keepdims=True))
        parts += [jnp.concatenate(sums, 0), jnp.concatenate(squares, 0)]
    row = across(jnp.concatenate(parts, 0))
    out_ref[...] = jnp.broadcast_to(row[None], out_ref.shape)


def shifted(slab, lane):
    before = jnp.where(lane == 0, 0.0, pltpu.roll(slab, 1, axis=1))
    after = jnp.where(lane == Z - 1, 0.0, pltpu.roll(slab, Z - 1, axis=1))
    return jnp.concatenate([before, slab, after], 0)


def lanes():
    return lax.broadcasted_iota(jnp.int32, (C, Z), 1)


def spread_kernel(one_ref, two_ref, up_ref, vol_ref, c1_ref, c2_ref, ug_ref, vol3_ref, *rest):
    sends, tmp = rest[:-1], rest[-1]
    lane = lanes()
    wanted = {}
    for n, side in enumerate(SIDES):
        for i, key in enumerate(slabs(side)):
            wanted.setdefault(key, []).append((n, i))
    for name, src, dst in (("c1", one_ref, c1_ref), ("c2", two_ref, c2_ref), ("ug", up_ref, ug_ref), ("vol", vol_ref, None)):
        tmp[...] = src[0].reshape(C * B * B, Z).astype(F32)
        for x in range(B):
            for y in range(B):
                slab = tmp[pl.ds(x * B + y, C, stride=B * B), :]
                if name == "vol":
                    vol3_ref[x, :, y * Z : (y + 1) * Z] = shifted(slab, lane).astype(BF16)
                    continue
                small = slab.astype(BF16)
                dst[x, :, y * Z : (y + 1) * Z] = small
                for n, i in wanted.get((name, x, y), ()):
                    sends[n][i] = small


def extend_kernel(pos_ref, c1_ref, c2_ref, ug_ref, vol3_ref, *rest):
    received = rest[:8]
    c1x_ref, c2x_ref, ugx_ref, r_ref, marks = rest[8:]
    for ref, own, w in ((c1x_ref, c1_ref, 1), (c2x_ref, c2_ref, 2), (ugx_ref, ug_ref, 2)):
        for x in range(B):
            ref[x + w, :, w * Z : (w + B) * Z] = own[x]
    target = {"c1": c1x_ref, "c2": c2x_ref, "ug": ugx_ref}
    for n, side in enumerate(SIDES):
        for i, (which, x, y) in enumerate(places(side)):
            target[which][x, :, y * Z : (y + 1) * Z] = received[n][i]
    sx, sy = pos_ref[0], pos_ref[1]
    row = lax.broadcasted_iota(jnp.int32, (16, B * Z), 0)
    gy = sy * B + lax.broadcasted_iota(jnp.int32, (16, B * Z), 1) // Z
    wy = gy + 1 - row % 3
    ok_y = (wy >= 0) & (wy < 4 * B) & (row < 9)

    def body(x, acc):
        wx = sx * B + x + 1 - row // 3
        ok = ok_y & (wx >= 0) & (wx < 4 * B)
        inside = jnp.where(ok, 1.0, 0.0).astype(BF16)
        parts = []
        for kx in range(3):
            for ky in range(3):
                parts.append(c1x_ref[x + 2 - kx, :, (2 - ky) * Z : (2 - ky + B) * Z])
        parts.append(inside)
        rhs = jnp.concatenate(parts, 0)
        return acc + lax.dot_general(
            vol3_ref[x], rhs, (((1,), (1,)), ((), ())), preferred_element_type=F32
        )

    acc = lax.fori_loop(0, B, body, jnp.zeros((3 * C, 9 * C + 16), F32))
    r_ref[...] = jnp.concatenate([acc, jnp.zeros((3 * C, 384 - 9 * C - 16), F32)], 1)


def moments(total, squares):
    mean = total * (1.0 / CELLS)
    inv = lax.rsqrt(squares * (1.0 / CELLS) - mean * mean + EPS)
    return mean, inv


def sigmoid(v):
    return 0.5 * jnp.tanh(0.5 * v) + 0.5


def silu_slope(v):
    s = sigmoid(v)
    return s * (1.0 + v * (1.0 - s))


def sums_two_kernel(got_ref, par_ref, c2_ref, ug_ref, out_ref, norm_ref, row_ref):
    row = arrived(got_ref)
    row_ref[...] = jnp.broadcast_to(row, (8, 128))
    cols = down(row)
    mean1, inv1 = moments(cols[0:32], cols[32:64])
    mean2, inv2 = moments(cols[64:96], cols[96:128])
    norm_ref[0], norm_ref[1], norm_ref[2], norm_ref[3] = mean1, inv1, mean2, inv2
    gain, bias = par_ref[64:96], par_ref[96:128]

    def body(x, acc):
        b, g = acc
        for y in range(B):
            cent = (c2_ref[x, :, y * Z : (y + 1) * Z].astype(F32) - mean2) * inv2
            up = ug_ref[x, :, y * Z : (y + 1) * Z].astype(F32)
            slope = up * silu_slope(gain * cent + bias)
            b, g = b + slope, g + slope * cent
        return b, g

    zero = jnp.zeros((C, Z), F32)
    b, g = lax.fori_loop(0, B, body, (zero, zero))
    out = across(jnp.concatenate([b, g, zero, zero], 0))
    out_ref[...] = jnp.broadcast_to(out[None], out_ref.shape)


def activation_kernel(norm_ref, par_ref, c1_ref, act3_ref):
    mean, inv = norm_ref[0], norm_ref[1]
    gain, bias = par_ref[0:32], par_ref[32:64]
    lane = lanes()

    def body(x, carry):
        for y in range(B):
            cent = (c1_ref[x, :, y * Z : (y + 1) * Z].astype(F32) - mean) * inv
            pre = gain * cent + bias
            act = (pre * sigmoid(pre)).astype(BF16).astype(F32)
            act3_ref[x, :, y * Z : (y + 1) * Z] = shifted(act, lane).astype(BF16)
        return carry

    lax.fori_loop(0, B, body, 0)


def edge(index, width, side, low, high):
    if index < width:
        return low
    if index >= width + B:
        return high
    return None


def windows(ref, x, first, y_first, count):
    parts = []
    for kx in range(3):
        for ky in range(3):
            parts.append(ref[x + first - kx, :, (y_first - ky) * Z : (y_first - ky + count) * Z])
    return jnp.concatenate(parts, 0)


def unshift(t, y, lane):
    left = t[0:C, y * Z : (y + 1) * Z]
    mid = t[C : 2 * C, y * Z : (y + 1) * Z]
    right = t[2 * C : 3 * C, y * Z : (y + 1) * Z]
    out = mid + jnp.where(lane == Z - 1, 0.0, pltpu.roll(left, Z - 1, axis=1))
    return out + jnp.where(lane == 0, 0.0, pltpu.roll(right, 1, axis=1))


def three(value):
    hi = value.astype(BF16).astype(F32)
    mid = (value - hi).astype(BF16).astype(F32)
    lo = value - hi - mid
    return hi, mid, lo


def middle_kernel(
    pos_ref, got_ref, norm_ref, par_ref, w_ref, c1x_ref, c2x_ref, ugx_ref, vol3_ref, act3_ref, r_ref,
    msg_ref, slope_ref, row_ref, grad, msg,
):
    sx, sy = pos_ref[0], pos_ref[1]
    row = arrived(got_ref)
    row_ref[...] = jnp.broadcast_to(row, (8, 128))
    cols = down(row)
    mean1, inv1, mean2, inv2 = norm_ref[0], norm_ref[1], norm_ref[2], norm_ref[3]
    gain1, bias1, gain2, bias2 = par_ref[0:32], par_ref[32:64], par_ref[64:96], par_ref[96:128]
    b2, g2 = cols[0:32] * (1.0 / CELLS), cols[32:64] * (1.0 / CELLS)
    amp = gain2 * inv2
    lane = lanes()
    inside_y = {
        y: jnp.where(sy > 0, 1.0, 0.0) if y < 2 else jnp.where(sy < 3, 1.0, 0.0)
        for y in (0, 1, B + 2, B + 3)
    }

    def first(x, carry):
        gx = sx * B + x - 2
        inside_x = jnp.where((gx >= 0) & (gx < 4 * B), 1.0, 0.0)
        amp_x = amp * inside_x
        for y in range(B + 4):
            cent = (c2x_ref[x, :, y * Z : (y + 1) * Z].astype(F32) - mean2) * inv2
            up = ugx_ref[x, :, y * Z : (y + 1) * Z].astype(F32)
            slope = up * silu_slope(gain2 * cent + bias2)
            a = amp_x * inside_y[y] if y in inside_y else amp_x
            grad[x, :, y * Z : (y + 1) * Z] = (a * (slope - b2 - cent * g2)).astype(BF16)
        return carry

    lax.fori_loop(0, B + 4, first, 0)
    inside_y = {0: jnp.where(sy > 0, 1.0, 0.0), B + 1: jnp.where(sy < 3, 1.0, 0.0)}

    def second(x, acc):
        b, g = acc
        gx = sx * B + x - 1
        inside_x = jnp.where((gx >= 0) & (gx < 4 * B), 1.0, 0.0)
        own_x = jnp.where((x >= 1) & (x <= B), 1.0, 0.0)
        t = jnp.dot(w_ref[...], windows(grad, x, 2, 2, B + 2), preferred_element_type=F32)
        bx, gsum = jnp.zeros((C, Z), F32), jnp.zeros((C, Z), F32)
        for y in range(B + 2):
            cent = (c1x_ref[x, :, y * Z : (y + 1) * Z].astype(F32) - mean1) * inv1
            slope = unshift(t, y, lane) * silu_slope(gain1 * cent + bias1)
            if 1 <= y <= B:
                bx, gsum = bx + slope, gsum + slope * cent
            inside = inside_x * inside_y[y] if y in inside_y else inside_x
            slope_ref[x, :, y * Z : (y + 1) * Z] = (slope * inside).astype(BF16)
        return b + bx * own_x, g + gsum * own_x

    zero = jnp.zeros((C, Z), F32)
    b, g = lax.fori_loop(0, B + 2, second, (zero, zero))

    def third(x, acc):
        s, f = acc
        dims = (((1,), (1,)), ((), ()))
        s = s + lax.dot_general(
            vol3_ref[x], windows(slope_ref, x, 2, 2, B), dims, preferred_element_type=F32
        )
        f = f + lax.dot_general(
            act3_ref[x], windows(grad, x, 3, 3, B), dims, preferred_element_type=F32
        )
        return s, f

    empty = jnp.zeros((3 * C, 9 * C), F32)
    s, f = lax.fori_loop(0, B, third, (empty, empty))
    pad = jnp.zeros((3 * C, 384 - 9 * C), F32)
    sums = across(jnp.concatenate([b, g, zero, zero], 0))
    hi, mid, lo = three(sums)
    for m, part in enumerate((jnp.concatenate([s, pad], 1), r_ref[...], jnp.concatenate([f, pad], 1))):
        for kz in range(3):
            for t in range(3):
                msg[:, m * 9 + kz * 3 + t, :] = part[kz * C : (kz + 1) * C, t * 128 : (t + 1) * 128]
    for i, part in enumerate((hi, mid, lo)):
        msg[:, 27 + i, :] = jnp.broadcast_to(part, (C, 128))
    msg[:, 30, :] = zero
    msg[:, 31, :] = zero
    msg_ref[...] = msg[...].astype(BF16)


def relay_kernel(got_ref, out_ref):
    total = jnp.sum(got_ref[...].astype(F32), axis=0)
    sums = total[27:28] + total[28:29] + total[29:30]
    hi, mid, lo = three(sums)
    out = jnp.concatenate([total[0:27], hi, mid, lo, total[30:32]], 0).astype(BF16)
    out_ref[...] = jnp.broadcast_to(out[None], out_ref.shape)


def share_kernel(got_ref, stat_ref, lanepar_ref, out_ref, row_ref):
    total = jnp.sum(got_ref[...].astype(F32), axis=0)
    sums = total[27:28] + total[28:29] + total[29:30]
    row_ref[...] = jnp.broadcast_to(sums, (8, 128))
    lane = lax.broadcasted_iota(jnp.int32, (1, 128), 1)
    stat = stat_ref[0:1]
    mean = stat * (1.0 / CELLS)
    squares = pltpu.roll(stat, 96, axis=1) * (1.0 / CELLS)
    inv = lax.rsqrt(jnp.where(lane < C, squares - mean * mean, 0.0) + EPS)
    g = pltpu.roll(sums, 96, axis=1)
    alpha = lanepar_ref[0:1] * inv
    gamma = alpha * inv * g * (1.0 / CELLS)
    delta = alpha * sums * (1.0 / CELLS) - gamma * mean
    rows = jnp.where(lane < C, jnp.concatenate([alpha, gamma, delta], 0), 0.0)
    rows = jnp.concatenate([rows, jnp.zeros((5, 128), F32)], 0)
    a = lax.broadcasted_iota(jnp.int32, (128, 384), 0)
    o = lax.broadcasted_iota(jnp.int32, (128, 384), 1)
    tile = jnp.where(o % C == a, 1.0, 0.0)
    wide = jnp.dot(rows, tile, precision=lax.Precision.HIGHEST, preferred_element_type=F32)
    spread = jnp.where((o // C + C == a) & (o < 9 * C), 1.0, 0.0)
    marks = jnp.concatenate([total[11:12], total[14:15], total[17:18], jnp.zeros((5, 128), F32)], 0)
    ones = jnp.dot(marks, spread, precision=lax.Precision.HIGHEST, preferred_element_type=F32)
    parts = []
    for kz in range(3):
        for t in range(3):
            cut = slice(t * 128, (t + 1) * 128)
            one = (
                wide[0:1, cut] * total[kz * 3 + t : kz * 3 + t + 1]
                - wide[1:2, cut] * total[9 + kz * 3 + t : 10 + kz * 3 + t]
                - wide[2:3, cut] * ones[kz : kz + 1, cut]
            )
            parts.append(one)
    out = jnp.concatenate(parts + [total[18:27], jnp.zeros((6, 128), F32)], 0) * SCALE
    out_ref[...] = jnp.broadcast_to(out.astype(BF16)[None], out_ref.shape)


def last_kernel(sum_ref, norm_ref, par_ref, w_ref, mask_ref, c1x_ref, slope_ref, out_ref, grad, tmp):
    cols = down(sum_ref[0:1])
    mean, inv = norm_ref[0], norm_ref[1]
    b, g = cols[0:32] * (1.0 / CELLS), cols[32:64] * (1.0 / CELLS)
    amp = par_ref[0:32] * inv
    lane = lanes()
    sx, sy = mask_ref[0], mask_ref[1]
    inside_y = {0: jnp.where(sy > 0, 1.0, 0.0), B + 1: jnp.where(sy < 3, 1.0, 0.0)}

    def first(x, carry):
        gx = sx * B + x - 1
        amp_x = amp * jnp.where((gx >= 0) & (gx < 4 * B), 1.0, 0.0)
        for y in range(B + 2):
            cent = (c1x_ref[x, :, y * Z : (y + 1) * Z].astype(F32) - mean) * inv
            slope = slope_ref[x, :, y * Z : (y + 1) * Z].astype(F32)
            a = amp_x * inside_y[y] if y in inside_y else amp_x
            grad[x, :, y * Z : (y + 1) * Z] = (a * (slope - b - cent * g)).astype(BF16)
        return carry

    lax.fori_loop(0, B + 2, first, 0)

    for x in range(B):
        t = jnp.dot(w_ref[...], windows(grad, x, 2, 2, B), preferred_element_type=F32)
        for y in range(B):
            tmp[pl.ds(x * B + y, C, stride=B * B), :] = unshift(t, y, lane)
    out_ref[0] = tmp[...].astype(BF16).reshape(C, B, B, Z)


def filters_kernel(got_ref, one_ref, two_ref, tmp):
    tmp[...] = got_ref[...].astype(F32)
    for m, ref in enumerate((one_ref, two_ref)):
        for kz in range(3):
            for t in range(3):
                slab = tmp[:, m * 9 + kz * 3 + t, :]
                for i in range(4):
                    k = 4 * t + i
                    if k < 9:
                        ref[k // 3, k % 3, kz] = slab[:, i * C : (i + 1) * C]


def exchanged(array, axes):
    return lax.all_to_all(array, axes, 0, 0, tiled=True)


def per_device(
    volume, conv_one, conv_two, upper_grad, weight_one, weight_two, gain_one, bias_one, gain_two, bias_two
):
    pos = jnp.stack([lax.axis_index("sx"), lax.axis_index("sy")]).astype(jnp.int32)
    packed = jnp.concatenate([gain_one, bias_one, gain_two, bias_two])
    par = jnp.broadcast_to(packed[:, None], (128, 128))
    lanepar = jnp.broadcast_to(packed[None, :], (8, 128))
    w_one = jnp.transpose(weight_one, (2, 3, 0, 1, 4)).reshape(3 * C, 9 * C)
    w_two = jnp.transpose(weight_two, (2, 3, 0, 1, 4)).reshape(3 * C, 9 * C)
    everyone = shaped((256, 1, 128), F32)

    stats = call(stats_kernel, everyone, n_in=2)(conv_one, conv_two)
    got_stats = exchanged(stats, ALL)

    block = shaped((B, C, B * Z), BF16)
    spread = call(
        spread_kernel,
        [block, block, block, shaped((B, 3 * C, B * Z), BF16)]
        + [shaped((len(slabs(side)), C, Z), BF16) for side in SIDES],
        scratch=[pltpu.VMEM((C * B * B, Z), F32)],
        flops=3 * 10**9,
        n_in=4,
    )(conv_one, conv_two, upper_grad, volume)
    c1, c2, ug, vol3 = spread[:4]
    received = []
    for n, (dx, dy) in enumerate(SIDES):
        pairs = []
        for x in range(4):
            for y in range(4):
                if 0 <= x + dx < 4 and 0 <= y + dy < 4:
                    pairs.append(((x + dx) * 4 + y + dy, x * 4 + y))
        message = spread[4 + SIDES.index((-dx, -dy))]
        received.append(lax.ppermute(message, ("sx", "sy"), pairs))
    c1x, c2x, ugx, r = call(
        extend_kernel,
        [
            shaped((B + 2, C, (B + 2) * Z), BF16),
            shaped((B + 4, C, (B + 4) * Z), BF16),
            shaped((B + 4, C, (B + 4) * Z), BF16),
            shaped((3 * C, 384), F32),
        ],
        scratch=[pltpu.VMEM((16, B * Z), BF16)],
        flops=3 * 10**9,
        n_smem=1,
        n_in=13,
    )(pos, c1, c2, ug, vol3, *received)

    sums_two, norm, stat_row = call(
        sums_two_kernel,
        [everyone, shaped((4, C, Z), F32), shaped((8, 128), F32)],
        flops=10**9,
        n_in=4,
    )(got_stats, par, c2, ug)
    got_two = exchanged(sums_two, ALL)
    act3 = call(activation_kernel, shaped((B, 3 * C, B * Z), BF16), flops=10**9, n_in=3)(norm, par, c1)

    terms, slope, row_two = call(
        middle_kernel,
        [
            shaped((32, 32, 128), BF16),
            shaped((B + 2, C, (B + 2) * Z), BF16),
            shaped((8, 128), F32),
        ],
        scratch=[pltpu.VMEM((B + 4, C, (B + 4) * Z), BF16), pltpu.VMEM((32, 32, 128), F32)],
        flops=4 * 10**9,
        n_smem=1,
        n_in=11,
    )(pos, got_two, norm, par, w_two, c1x, c2x, ugx, vol3, act3, r)

    relay = call(relay_kernel, shaped((8, 32, 128), BF16), n_in=1)(exchanged(terms, PLANE))
    shares, row_one = call(
        share_kernel, [shaped((32, 24, 128), BF16), shaped((8, 128), F32)], n_in=3
    )(exchanged(relay, "dp_0"), stat_row, lanepar)
    got_shares = exchanged(shares, PLANE)
    input_grad = call(
        lambda sum_ref, *refs: last_kernel(sum_ref, *refs[0:3], refs[3], *refs[4:]),
        shaped((1, C, B, B, Z), BF16),
        scratch=[pltpu.VMEM((B + 2, C, (B + 2) * Z), BF16), pltpu.VMEM((C * B * B, Z), F32)],
        flops=4 * 10**9,
        n_in=7,
    ) if False else None
    input_grad = pl.pallas_call(
        last_kernel,
        out_shape=shaped((1, C, B, B, Z), BF16),
        in_specs=[pl.BlockSpec(memory_space=VMEM)] * 4
        + [pl.BlockSpec(memory_space=SMEM)]
        + [pl.BlockSpec(memory_space=VMEM)] * 2,
        out_specs=pl.BlockSpec(memory_space=VMEM),
        scratch_shapes=[pltpu.VMEM((B + 2, C, (B + 2) * Z), BF16), pltpu.VMEM((C * B * B, Z), F32)],
        compiler_params=pltpu.CompilerParams(vmem_limit_bytes=40 * 2**20),
        cost_estimate=pl.CostEstimate(flops=4 * 10**9, bytes_accessed=1 << 20, transcendentals=0),
    )(row_one, norm, par, w_one, pos, c1x, slope)
    filters = shaped((3, 3, 3, C, C), F32)
    filter_one, filter_two = call(
        filters_kernel, [filters, filters], scratch=[pltpu.VMEM((32, 24, 128), F32)], n_in=1
    )(got_shares)
    one = row_one[0] * SCALE
    two = row_two[0] * SCALE
    return (input_grad, filter_one, filter_two, one[32:64], one[0:32], two[32:64], two[0:32])


def solution(mesh):
    finer = Mesh(
        mesh.devices.reshape(8, 2, mesh.shape["sx"], mesh.shape["sy"]), ("dp_0", "dp_1", "sx", "sy")
    )
    field = P(DP, None, "sx", "sy", None)
    return jax.shard_map(
        per_device,
        mesh=finer,
        in_specs=(field,) * 4 + (P(),) * 6,
        out_specs=(field,) + (P(),) * 6,
        check_vma=False,
    )
```

```python
import math

import jax
import jax.numpy as jnp
from jax import lax
from jax.experimental import pallas as pl
from jax.experimental.pallas import tpu as pltpu
from jax.sharding import Mesh
from jax.sharding import PartitionSpec as P

DP = ("dp_0", "dp_1")
ALL = ("dp_0", "dp_1", "sx", "sy")
PLANE = ("dp_1", "sx", "sy")
EPS = 1e-05
F32 = jnp.float32
BF16 = jnp.bfloat16
C = 32
B = 8
Z = 128
CELLS = float(16 * 32 * 32 * Z)
SCALE = 1.0 / math.sqrt(CELLS)

VMEM = pltpu.MemorySpace.VMEM
SMEM = pltpu.MemorySpace.SMEM
HBM = pltpu.MemorySpace.HBM
FIELDS = (("c2", 2), ("ug", 2), ("c1", 1))


def span(side, width):
    return range(B - width, B) if side > 0 else range(width)


def landing(side, width):
    return range(B + width, B + 2 * width) if side > 0 else range(width)


def layers_x(side):
    return [(f, x) for f, w in FIELDS for x in span(side, w)]


def places_x(side):
    return [(f, x) for f, w in FIELDS for x in landing(side, w)]


def slabs_y(side):
    return [(f, y, x) for f, w in FIELDS for y in span(side, w) for x in range(B + 2 * w)]


def places_y(side):
    runs, first = [], 0
    for f, w in FIELDS:
        for y in landing(side, w):
            runs.append((first, B + 2 * w, f, y))
            first += B + 2 * w
    return runs


def call(kernel, outs, scratch=(), flops=0, spaces=(), limit=6, homes=None):
    single = not isinstance(outs, (list, tuple))
    shapes = [outs] if single else list(outs)
    homes = homes or [VMEM] * len(shapes)
    specs = [pl.BlockSpec(memory_space=space) for space in homes]
    shapes = [HBM(x.shape, x.dtype) if home == HBM else x for x, home in zip(shapes, homes)]
    f = pl.pallas_call(
        kernel,
        out_shape=shapes[0] if single else tuple(shapes),
        in_specs=[pl.BlockSpec(memory_space=space) for space in spaces],
        out_specs=specs[0] if single else tuple(specs),
        scratch_shapes=list(scratch),
        compiler_params=pltpu.CompilerParams(vmem_limit_bytes=limit * 2**20),
        cost_estimate=pl.CostEstimate(flops=flops, bytes_accessed=1 << 20, transcendentals=0),
    )

    def placed(*arguments):
        return f(
            *[
                pltpu.with_memory_space_constraint(x, HBM) if space == HBM else x
                for x, space in zip(arguments, spaces)
            ]
        )

    return placed


def started(pairs, sems):
    copies = [pltpu.make_async_copy(src, dst, sems.at[n]) for n, (src, dst) in enumerate(pairs)]
    for copy in copies:
        copy.start()
    return copies


def shaped(dims, kind):
    return jax.ShapeDtypeStruct(dims, kind)


def across(columns):
    return jnp.sum(jnp.transpose(columns), axis=0, keepdims=True)


def down(row):
    return jnp.transpose(jnp.broadcast_to(row, (128, 128)))


def arrived(ref):
    total = jnp.sum(ref[...].reshape(ref.shape[0], 128), axis=0, keepdims=True)
    return total


def shifted(slab, lane):
    before = jnp.where(lane == 0, 0.0, pltpu.roll(slab, 1, axis=1))
    after = jnp.where(lane == Z - 1, 0.0, pltpu.roll(slab, Z - 1, axis=1))
    return jnp.concatenate([before, slab, after], 0)


def lanes():
    return lax.broadcasted_iota(jnp.int32, (C, Z), 1)


def spread_kernel(
    one_ref, two_ref, up_ref, vol_ref, c1_ref, c2_ref, ug_ref, vol3_out, down_ref, up_x_ref, stat_ref,
    held, tmp, vol3, sems, out_sem,
):
    sources = (("vol", vol_ref, None), ("c1", one_ref, c1_ref), ("c2", two_ref, c2_ref), ("ug", up_ref, ug_ref))
    copies = started([(src.at[0], held.at[n]) for n, (_, src, _) in enumerate(sources)], sems)
    lane = lanes()
    parts = []
    for n, (name, _, dst) in enumerate(sources):
        copies[n].wait()
        tmp[...] = held[n].reshape(C * B * B, Z).astype(F32)
        total, squares = jnp.zeros((C, Z), F32), jnp.zeros((C, Z), F32)
        for x in range(B):
            for y in range(B):
                slab = tmp[pl.ds(x * B + y, C, stride=B * B), :]
                if name == "vol":
                    vol3[x, :, y * Z : (y + 1) * Z] = shifted(slab, lane).astype(BF16)
                    continue
                if name in ("c1", "c2"):
                    total, squares = total + slab, squares + slab * slab
                dst[x, :, y * Z : (y + 1) * Z] = slab.astype(BF16)
        if name == "vol":
            leaving = pltpu.make_async_copy(vol3, vol3_out, out_sem.at[0])
            leaving.start()
        if name in ("c1", "c2"):
            parts += [total, squares]
    own = {"c1": c1_ref, "c2": c2_ref, "ug": ug_ref}
    for side, ref in ((-1, down_ref), (1, up_x_ref)):
        for i, (f, x) in enumerate(layers_x(side)):
            ref[i] = own[f][x]
    row = across(jnp.concatenate(parts, 0))
    stat_ref[...] = jnp.broadcast_to(row[None], stat_ref.shape)
    leaving.wait()


def pack_kernel(c1_ref, c2_ref, ug_ref, low_ref, high_ref, down_ref, up_ref):
    where = {}
    for f, w, ref in (("c1", 1, c1_ref), ("c2", 2, c2_ref), ("ug", 2, ug_ref)):
        for x in range(B):
            where[(f, x + w)] = (ref, x)
    for side, ref in ((-1, low_ref), (1, high_ref)):
        for i, key in enumerate(places_x(side)):
            where[key] = (ref, i)
    for side, out in ((-1, down_ref), (1, up_ref)):
        for i, (f, y, x) in enumerate(slabs_y(side)):
            ref, n = where[(f, x)]
            out[i] = ref[n, :, y * Z : (y + 1) * Z]


def extend_kernel(
    pos_ref, stat_ref, par_ref, c1_ref, c2_ref, slope_ref, xlow_ref, xhigh_ref, vol3_in, ylow_in, yhigh_in,
    c1x_out, c2x_out, slopex_out, turn_out, act3_out, r_ref, c1x, c2x, slopex, turn, act3, ugx, vol3, sems, out_sems,
):
    target = {"c1": c1x, "c2": c2x, "ug": ugx}
    pairs = []
    for side, ref in ((-1, ylow_in), (1, yhigh_in)):
        for first, count, f, y in places_y(side):
            pairs.append((ref.at[pl.ds(first, count)], target[f].at[:, :, pl.ds(y * Z, Z)]))
    pairs.append((vol3_in, vol3))
    arriving = started(pairs, sems)
    (mean1, inv1), (mean2, inv2) = norms(stat_ref)
    gain1, bias1, gain2, bias2 = par_ref[0:32], par_ref[32:64], par_ref[64:96], par_ref[96:128]
    lane = lanes()

    def activation(x, carry):
        for y in range(B):
            cut = slice(y * Z, (y + 1) * Z)
            cent = (c1_ref[x, :, cut].astype(F32) - mean1) * inv1
            pre = gain1 * cent + bias1
            s = sigmoid(pre)
            act3[x, :, cut] = shifted((pre * s).astype(BF16).astype(F32), lane).astype(BF16)
            turn[x + 1, :, (y + 1) * Z : (y + 2) * Z] = s * (1.0 + pre * (1.0 - s))
        return carry

    lax.fori_loop(0, B, activation, 0)
    leaving = started([(act3, act3_out)], out_sems)
    for f, w, own in (("c1", 1, c1_ref), ("c2", 2, c2_ref)):
        for x in range(B):
            target[f][x + w, :, w * Z : (w + B) * Z] = own[x]
    width = dict(FIELDS)
    for side, ref in ((-1, xlow_ref), (1, xhigh_ref)):
        for i, (f, x) in enumerate(places_x(side)):
            w = width[f]
            target[f][x, :, w * Z : (w + B) * Z] = ref[i]
    for copy in arriving:
        copy.wait()
    leaving += started([(c1x, c1x_out), (c2x, c2x_out)], out_sems.at[pl.ds(1, 2)])

    def slope_at(x, y):
        cut = slice(y * Z, (y + 1) * Z)
        cent = (c2x[x, :, cut].astype(F32) - mean2) * inv2
        slopex[x, :, cut] = ugx[x, :, cut].astype(F32) * silu_slope(gain2 * cent + bias2)

    def ends(i, carry):
        x = jnp.where(i < 2, i, i + B)
        for y in range(B + 4):
            slope_at(x, y)
        return carry

    lax.fori_loop(0, 4, ends, 0)

    def between(x, carry):
        for y in (0, 1, B + 2, B + 3):
            slope_at(x + 2, y)
        slopex[x + 2, :, 2 * Z : (2 + B) * Z] = slope_ref[x]
        return carry

    lax.fori_loop(0, B, between, 0)
    leaving += started([(slopex, slopex_out)], out_sems.at[pl.ds(3, 1)])

    def turn_at(x, y):
        cut = slice(y * Z, (y + 1) * Z)
        cent = (c1x[x, :, cut].astype(F32) - mean1) * inv1
        turn[x, :, cut] = silu_slope(gain1 * cent + bias1)

    for x in (0, B + 1):
        for y in range(B + 2):
            turn_at(x, y)

    def sides(x, carry):
        turn_at(x + 1, 0)
        turn_at(x + 1, B + 1)
        return carry

    lax.fori_loop(0, B, sides, 0)
    leaving += started([(turn, turn_out)], out_sems.at[pl.ds(4, 1)])

    sx, sy = pos_ref[0], pos_ref[1]
    row = lax.broadcasted_iota(jnp.int32, (16, B * Z), 0)
    gy = sy * B + lax.broadcasted_iota(jnp.int32, (16, B * Z), 1) // Z
    wy = gy + 1 - row % 3
    ok_y = (wy >= 0) & (wy < 4 * B) & (row < 9)

    def body(x, acc):
        wx = sx * B + x + 1 - row // 3
        inside = jnp.where(ok_y & (wx >= 0) & (wx < 4 * B), 1.0, 0.0).astype(BF16)
        lhs = jnp.concatenate([windows(c1x, x, 2, 2, B), inside], 0)
        return acc + lax.dot_general(lhs, vol3[x], TRANSPOSED, preferred_element_type=F32)

    acc = lax.fori_loop(0, B, body, jnp.zeros((9 * C + 16, 3 * C), F32))
    r_ref[...] = turned(acc).astype(BF16)
    for copy in leaving:
        copy.wait()


TRANSPOSED = (((1,), (1,)), ((), ()))


def turned(acc):
    rows = acc.shape[0]
    full = jnp.concatenate([acc, jnp.zeros((384 - rows, 3 * C), F32)], 0)
    full = jnp.concatenate([full, jnp.zeros((384, 128 - 3 * C), F32)], 1)
    return jnp.concatenate([jnp.transpose(full[i * 128 : (i + 1) * 128]) for i in range(3)], 1)


def moments(total, squares):
    mean = total * (1.0 / CELLS)
    inv = lax.rsqrt(squares * (1.0 / CELLS) - mean * mean + EPS)
    return mean, inv


def norms(stat_ref):
    cols = down(stat_ref[0:1])
    return moments(cols[0:32], cols[32:64]), moments(cols[64:96], cols[96:128])


def sigmoid(v):
    return 0.5 * jnp.tanh(0.5 * v) + 0.5


def silu_slope(v):
    s = sigmoid(v)
    return s * (1.0 + v * (1.0 - s))


def sums_two_kernel(got_ref, par_ref, c2_ref, ug_ref, out_ref, row_ref, slope_ref):
    row = arrived(got_ref)
    row_ref[...] = jnp.broadcast_to(row, (8, 128))
    _, (mean2, inv2) = norms(row_ref)
    gain, bias = par_ref[64:96], par_ref[96:128]

    def body(x, acc):
        b, g = acc
        for y in range(B):
            cent = (c2_ref[x, :, y * Z : (y + 1) * Z].astype(F32) - mean2) * inv2
            up = ug_ref[x, :, y * Z : (y + 1) * Z].astype(F32)
            slope = up * silu_slope(gain * cent + bias)
            slope_ref[x, :, y * Z : (y + 1) * Z] = slope
            b, g = b + slope, g + slope * cent
        return b, g

    zero = jnp.zeros((C, Z), F32)
    b, g = lax.fori_loop(0, B, body, (zero, zero))
    out = across(jnp.concatenate([b, g, zero, zero], 0))
    out_ref[...] = jnp.broadcast_to(out[None], out_ref.shape)


def windows(ref, x, first, y_first, count):
    parts = []
    for kx in range(3):
        for ky in range(3):
            parts.append(ref[x + first - kx, :, (y_first - ky) * Z : (y_first - ky + count) * Z])
    return jnp.concatenate(parts, 0)


def unshift(t, y, lane):
    left = t[0:C, y * Z : (y + 1) * Z]
    mid = t[C : 2 * C, y * Z : (y + 1) * Z]
    right = t[2 * C : 3 * C, y * Z : (y + 1) * Z]
    out = mid + jnp.where(lane == Z - 1, 0.0, pltpu.roll(left, Z - 1, axis=1))
    return out + jnp.where(lane == 0, 0.0, pltpu.roll(right, 1, axis=1))


def as_matrix(src, dst):
    for kz in range(3):
        parts = [src[kx, ky, kz].astype(F32) for kx in range(3) for ky in range(3)]
        dst[kz * C : (kz + 1) * C, :] = jnp.concatenate(parts, 1).astype(BF16)


def three(value):
    hi = value.astype(BF16).astype(F32)
    mid = (value - hi).astype(BF16).astype(F32)
    lo = value - hi - mid
    return hi, mid, lo


def middle_kernel(
    pos_ref, got_ref, stat_ref, par_ref, w_in, c1x_in, c2x_in, slopex_in, turn_in, vol3_in, act3_in, r_in,
    msg_ref, slope_ref, row_ref, w_ref, c1x_ref, c2x_ref, slopex_ref, turn_ref, vol3_ref, act3_ref, r_ref,
    raw, grad, msg, sems,
):
    arriving = started(
        [
            (slopex_in, slopex_ref),
            (c2x_in, c2x_ref),
            (w_in, raw),
            (turn_in, turn_ref),
            (c1x_in, c1x_ref),
            (vol3_in, vol3_ref),
            (act3_in, act3_ref),
            (r_in, r_ref),
        ],
        sems,
    )
    sx, sy = pos_ref[0], pos_ref[1]
    row = arrived(got_ref)
    row_ref[...] = jnp.broadcast_to(row, (8, 128))
    cols = down(row)
    (mean1, inv1), (mean2, inv2) = norms(stat_ref)
    amp = par_ref[64:96] * inv2
    by = amp * inv2 * cols[32:64] * (1.0 / CELLS)
    off = amp * cols[0:32] * (1.0 / CELLS) - by * mean2
    lane = lanes()
    inside_y = {
        y: jnp.where(sy > 0, 1.0, 0.0) if y < 2 else jnp.where(sy < 3, 1.0, 0.0)
        for y in (0, 1, B + 2, B + 3)
    }

    def first(x, carry):
        gx = sx * B + x - 2
        inside_x = jnp.where((gx >= 0) & (gx < 4 * B), 1.0, 0.0)
        for y in range(B + 4):
            cut = slice(y * Z, (y + 1) * Z)
            value = amp * slopex_ref[x, :, cut] - by * c2x_ref[x, :, cut].astype(F32) - off
            keep = inside_x * inside_y[y] if y in inside_y else inside_x
            grad[x, :, cut] = (value * keep).astype(BF16)
        return carry

    arriving[0].wait()
    arriving[1].wait()
    lax.fori_loop(0, B + 4, first, 0)
    arriving[2].wait()
    as_matrix(raw, w_ref)
    arriving[3].wait()
    arriving[4].wait()
    inside_y = {0: jnp.where(sy > 0, 1.0, 0.0), B + 1: jnp.where(sy < 3, 1.0, 0.0)}

    def second(x, acc):
        b, g = acc
        gx = sx * B + x - 1
        inside_x = jnp.where((gx >= 0) & (gx < 4 * B), 1.0, 0.0)
        own_x = jnp.where((x >= 1) & (x <= B), 1.0, 0.0)
        t = jnp.dot(w_ref[...], windows(grad, x, 2, 2, B + 2), preferred_element_type=F32)
        bx, gsum = jnp.zeros((C, Z), F32), jnp.zeros((C, Z), F32)
        for y in range(B + 2):
            cut = slice(y * Z, (y + 1) * Z)
            slope = unshift(t, y, lane) * turn_ref[x, :, cut]
            if 1 <= y <= B:
                bx, gsum = bx + slope, gsum + slope * c1x_ref[x, :, cut].astype(F32)
            inside = inside_x * inside_y[y] if y in inside_y else inside_x
            slope_ref[x, :, cut] = (slope * inside).astype(BF16)
        gsum = (gsum - mean1 * bx) * inv1
        return b + bx * own_x, g + gsum * own_x

    zero = jnp.zeros((C, Z), F32)
    b, g = lax.fori_loop(0, B + 2, second, (zero, zero))

    def third(x, acc):
        s, f = acc
        s = s + lax.dot_general(windows(slope_ref, x, 2, 2, B), vol3_ref[x], TRANSPOSED, preferred_element_type=F32)
        f = f + lax.dot_general(windows(grad, x, 3, 3, B), act3_ref[x], TRANSPOSED, preferred_element_type=F32)
        return s, f

    for copy in arriving[5:]:
        copy.wait()
    empty = jnp.zeros((9 * C, 3 * C), F32)
    s, f = lax.fori_loop(0, B, third, (empty, empty))
    sums = across(jnp.concatenate([b, g, zero, zero], 0))
    hi, mid, lo = three(sums)
    for m, part in enumerate((turned(s), r_ref[...].astype(F32), turned(f))):
        for kz in range(3):
            for t in range(3):
                msg[:, m * 9 + kz * 3 + t, :] = part[kz * C : (kz + 1) * C, t * 128 : (t + 1) * 128]
    for i, part in enumerate((hi, mid, lo)):
        msg[:, 27 + i, :] = jnp.broadcast_to(part, (C, 128))
    msg[:, 30, :] = zero
    msg[:, 31, :] = zero
    msg_ref[...] = msg[...].astype(BF16)


def relay_kernel(got_ref, out_ref):
    total = jnp.sum(got_ref[...].astype(F32), axis=0)
    sums = total[27:28] + total[28:29] + total[29:30]
    hi, mid, lo = three(sums)
    out = jnp.concatenate([total[0:27], hi, mid, lo, total[30:32]], 0).astype(BF16)
    out_ref[...] = jnp.broadcast_to(out[None], out_ref.shape)


def share_kernel(got_ref, stat_ref, lanepar_ref, out_ref, row_ref):
    total = jnp.sum(got_ref[...].astype(F32), axis=0)
    sums = total[27:28] + total[28:29] + total[29:30]
    row_ref[...] = jnp.broadcast_to(sums, (8, 128))
    lane = lax.broadcasted_iota(jnp.int32, (1, 128), 1)
    stat = stat_ref[0:1]
    mean = stat * (1.0 / CELLS)
    squares = pltpu.roll(stat, 96, axis=1) * (1.0 / CELLS)
    inv = lax.rsqrt(jnp.where(lane < C, squares - mean * mean, 0.0) + EPS)
    g = pltpu.roll(sums, 96, axis=1)
    alpha = lanepar_ref[0:1] * inv
    gamma = alpha * inv * g * (1.0 / CELLS)
    delta = alpha * sums * (1.0 / CELLS) - gamma * mean
    rows = jnp.where(lane < C, jnp.concatenate([alpha, gamma, delta], 0), 0.0)
    rows = jnp.concatenate([rows, jnp.zeros((5, 128), F32)], 0)
    a = lax.broadcasted_iota(jnp.int32, (128, 384), 0)
    o = lax.broadcasted_iota(jnp.int32, (128, 384), 1)
    tile = jnp.where(o % C == a, 1.0, 0.0)
    wide = jnp.dot(rows, tile, precision=lax.Precision.HIGHEST, preferred_element_type=F32)
    spread = jnp.where((o // C + C == a) & (o < 9 * C), 1.0, 0.0)
    marks = jnp.concatenate([total[11:12], total[14:15], total[17:18], jnp.zeros((5, 128), F32)], 0)
    ones = jnp.dot(marks, spread, precision=lax.Precision.HIGHEST, preferred_element_type=F32)
    parts = []
    for kz in range(3):
        for t in range(3):
            cut = slice(t * 128, (t + 1) * 128)
            one = (
                wide[0:1, cut] * total[kz * 3 + t : kz * 3 + t + 1]
                - wide[1:2, cut] * total[9 + kz * 3 + t : 10 + kz * 3 + t]
                - wide[2:3, cut] * ones[kz : kz + 1, cut]
            )
            parts.append(one)
    out = jnp.concatenate(parts + [total[18:27], jnp.zeros((6, 128), F32)], 0) * SCALE
    out_ref[...] = jnp.broadcast_to(out.astype(BF16)[None], out_ref.shape)


def last_kernel(
    mask_ref, sum_ref, two_ref, stat_ref, par_ref, slope_ref, w_in, c1x_in,
    out_ref, gain1_ref, bias1_ref, gain2_ref, bias2_ref, grad, tmp, w_ref, raw, c1x_ref, sems,
):
    arriving = started([(w_in, raw), (c1x_in, c1x_ref)], sems)
    for ref, bias_ref, gain_ref in ((sum_ref, bias1_ref, gain1_ref), (two_ref, bias2_ref, gain2_ref)):
        scaled = ref[0:1] * SCALE
        bias_ref[...] = scaled[:, 0:C]
        gain_ref[...] = pltpu.roll(scaled, 96, axis=1)[:, 0:C]
    cols = down(sum_ref[0:1])
    (mean, inv), _ = norms(stat_ref)
    b, g = cols[0:32] * (1.0 / CELLS), cols[32:64] * (1.0 / CELLS)
    amp = par_ref[0:32] * inv
    by = amp * inv * g
    off = amp * b - by * mean
    lane = lanes()
    sx, sy = mask_ref[0], mask_ref[1]
    inside_y = {0: jnp.where(sy > 0, 1.0, 0.0), B + 1: jnp.where(sy < 3, 1.0, 0.0)}

    def first(x, carry):
        gx = sx * B + x - 1
        inside_x = jnp.where((gx >= 0) & (gx < 4 * B), 1.0, 0.0)
        for y in range(B + 2):
            cut = slice(y * Z, (y + 1) * Z)
            value = amp * slope_ref[x, :, cut].astype(F32) - by * c1x_ref[x, :, cut].astype(F32) - off
            keep = inside_x * inside_y[y] if y in inside_y else inside_x
            grad[x, :, cut] = (value * keep).astype(BF16)
        return carry

    for copy in arriving:
        copy.wait()
    as_matrix(raw, w_ref)
    lax.fori_loop(0, B + 2, first, 0)

    for x in range(B):
        t = jnp.dot(w_ref[...], windows(grad, x, 2, 2, B), preferred_element_type=F32)
        for y in range(B):
            tmp[pl.ds(x * B + y, C, stride=B * B), :] = unshift(t, y, lane)
    out_ref[0] = tmp[...].astype(BF16).reshape(C, B, B, Z)


def filters_kernel(got_ref, one_ref, two_ref, tmp):
    tmp[...] = got_ref[...].astype(F32)
    for m, ref in enumerate((one_ref, two_ref)):
        for kz in range(3):
            for t in range(3):
                slab = tmp[:, m * 9 + kz * 3 + t, :]
                for i in range(4):
                    k = 4 * t + i
                    if k < 9:
                        ref[k // 3, k % 3, kz] = slab[:, i * C : (i + 1) * C]


def exchanged(array, axes):
    return lax.all_to_all(array, axes, 0, 0, tiled=True)


def per_device(
    volume, conv_one, conv_two, upper_grad, weight_one, weight_two, gain_one, bias_one, gain_two, bias_two
):
    pos = jnp.stack([lax.axis_index("sx"), lax.axis_index("sy")]).astype(jnp.int32)
    packed = jnp.concatenate([gain_one, bias_one, gain_two, bias_two])
    par = jnp.broadcast_to(packed[:, None], (128, 128))
    lanepar = jnp.broadcast_to(packed[None, :], (8, 128))
    everyone = shaped((256, 1, 128), F32)
    block = shaped((B, C, B * Z), BF16)
    three_fold = shaped((B, 3 * C, B * Z), BF16)
    near = shaped((B + 2, C, (B + 2) * Z), BF16)
    far = shaped((B + 4, C, (B + 4) * Z), BF16)
    weights = shaped((3, 3, 3, C, C), BF16)
    near_wide, far_wide, block_wide = (shaped(a.shape, F32) for a in (near, far, block))
    row = shaped((8, 128), F32)

    def room(like):
        return pltpu.VMEM(like.shape, like.dtype)

    def sems(count):
        return pltpu.SemaphoreType.DMA((count,))

    along_x = shaped((len(layers_x(1)), C, B * Z), BF16)
    c1, c2, ug, vol3, send_down, send_up, stats = call(
        spread_kernel,
        [block, block, block, three_fold, along_x, along_x, everyone],
        scratch=[
            pltpu.VMEM((4, C, B, B, Z), BF16),
            pltpu.VMEM((C * B * B, Z), F32),
            room(three_fold),
            sems(4),
            sems(1),
        ],
        spaces=[HBM] * 4,
        homes=[VMEM] * 3 + [HBM] + [VMEM] * 3,
        limit=10,
    )(conv_one, conv_two, upper_grad, volume)
    up = [(i, i + 1) for i in range(3)]
    down_ = [(i + 1, i) for i in range(3)]
    x_low = lax.ppermute(send_up, "sx", up)
    x_high = lax.ppermute(send_down, "sx", down_)
    got_stats = exchanged(stats, ALL)
    along_y = shaped((len(slabs_y(1)), C, Z), BF16)
    send_down, send_up = call(pack_kernel, [along_y, along_y], spaces=[VMEM] * 5)(c1, c2, ug, x_low, x_high)
    y_low = lax.ppermute(send_up, "sy", up)
    y_high = lax.ppermute(send_down, "sy", down_)

    sums_two, stat_row, slope_two = call(
        sums_two_kernel, [everyone, row, block_wide], spaces=[VMEM] * 4
    )(got_stats, par, c2, ug)
    got_two = exchanged(sums_two, ALL)
    r_shape = shaped((128, 384), BF16)
    c1x, c2x, slopex, turn, act3, r = call(
        extend_kernel,
        [near, far, far_wide, near_wide, three_fold, r_shape],
        scratch=[
            room(near), room(far), room(far_wide), room(near_wide), room(three_fold), room(far), room(three_fold), sems(11), sems(5)
        ],
        flops=5 * 10**9,
        spaces=[SMEM] + [VMEM] * 7 + [HBM] * 3,
        homes=[HBM] * 5 + [VMEM],
        limit=16,
    )(pos, stat_row, par, c1, c2, slope_two, x_low, x_high, vol3, y_low, y_high)

    terms, slope, row_two = call(
        middle_kernel,
        [shaped((32, 32, 128), BF16), near, row],
        scratch=[
            pltpu.VMEM((3 * C, 9 * C), BF16), room(near), room(far), room(far_wide), room(near_wide), room(three_fold),
            room(three_fold), room(r_shape), room(weights), room(far), pltpu.VMEM((32, 32, 128), F32), sems(8),
        ],
        flops=4 * 10**9,
        spaces=[SMEM] + [VMEM] * 3 + [HBM] * 8,
        limit=18,
    )(pos, got_two, stat_row, par, weight_two, c1x, c2x, slopex, turn, vol3, act3, r)

    got_terms = exchanged(terms, PLANE)
    relay = call(relay_kernel, shaped((8, 32, 128), BF16), spaces=[VMEM])(got_terms)
    got_relay = exchanged(relay, "dp_0")
    shares, row_one = call(
        share_kernel, [shaped((32, 24, 128), BF16), row], spaces=[VMEM] * 3
    )(got_relay, stat_row, lanepar)
    got_shares = exchanged(shares, PLANE)
    vector = shaped((1, C), F32)
    input_grad, gain_one_grad, bias_one_grad, gain_two_grad, bias_two_grad = call(
        last_kernel,
        [shaped((1, C, B, B, Z), BF16), vector, vector, vector, vector],
        scratch=[
            room(near), pltpu.VMEM((C * B * B, Z), F32), pltpu.VMEM((3 * C, 9 * C), BF16), room(weights), room(near), sems(2)
        ],
        flops=4 * 10**9,
        spaces=[SMEM] + [VMEM] * 5 + [HBM] * 2,
        limit=10,
    )(pos, row_one, row_two, stat_row, par, slope, weight_one, c1x)
    filters = shaped((3, 3, 3, C, C), F32)
    filter_one, filter_two = call(
        filters_kernel, [filters, filters], scratch=[pltpu.VMEM((32, 24, 128), F32)], spaces=[VMEM]
    )(got_shares)
    return (
        input_grad, filter_one, filter_two, gain_one_grad[0], bias_one_grad[0], gain_two_grad[0], bias_two_grad[0]
    )


def solution(mesh):
    finer = Mesh(
        mesh.devices.reshape(8, 2, mesh.shape["sx"], mesh.shape["sy"]), ("dp_0", "dp_1", "sx", "sy")
    )
    field = P(DP, None, "sx", "sy", None)
    return jax.shard_map(
        per_device,
        mesh=finer,
        in_specs=(field,) * 4 + (P(),) * 6,
        out_specs=(field,) + (P(),) * 6,
        check_vma=False,
    )
```

```python
import math

import jax
import jax.numpy as jnp
from jax import lax
from jax.experimental import pallas as pl
from jax.experimental.pallas import tpu as pltpu
from jax.sharding import Mesh
from jax.sharding import PartitionSpec as P

DP = ("dp_0", "dp_1")
ALL = ("dp_0", "dp_1", "sx", "sy")
PLANE = ("dp_1", "sx", "sy")
EPS = 1e-05
F32 = jnp.float32
BF16 = jnp.bfloat16
C = 32
B = 8
Z = 128
CELLS = float(16 * 32 * 32 * Z)
SCALE = 1.0 / math.sqrt(CELLS)

VMEM = pltpu.MemorySpace.VMEM
SMEM = pltpu.MemorySpace.SMEM
HBM = pltpu.MemorySpace.HBM
FIELDS = (("c2", 2), ("ug", 2), ("c1", 1))


def span(side, width):
    return range(B - width, B) if side > 0 else range(width)


def landing(side, width):
    return range(B + width, B + 2 * width) if side > 0 else range(width)


def layers_x(side):
    return [(f, x) for f, w in FIELDS for x in span(side, w)]


def places_x(side):
    return [(f, x) for f, w in FIELDS for x in landing(side, w)]


def slabs_y(side):
    return [(f, y, x) for f, w in FIELDS for y in span(side, w) for x in range(B + 2 * w)]


def places_y(side):
    runs, first = [], 0
    for f, w in FIELDS:
        for y in landing(side, w):
            runs.append((first, B + 2 * w, f, y))
            first += B + 2 * w
    return runs


def call(kernel, outs, scratch=(), flops=0, spaces=(), limit=6, homes=None):
    single = not isinstance(outs, (list, tuple))
    shapes = [outs] if single else list(outs)
    homes = homes or [VMEM] * len(shapes)
    specs = [pl.BlockSpec(memory_space=space) for space in homes]
    shapes = [HBM(x.shape, x.dtype) if home == HBM else x for x, home in zip(shapes, homes)]
    f = pl.pallas_call(
        kernel,
        out_shape=shapes[0] if single else tuple(shapes),
        in_specs=[pl.BlockSpec(memory_space=space) for space in spaces],
        out_specs=specs[0] if single else tuple(specs),
        scratch_shapes=list(scratch),
        compiler_params=pltpu.CompilerParams(vmem_limit_bytes=limit * 2**20),
        cost_estimate=pl.CostEstimate(flops=flops, bytes_accessed=1 << 20, transcendentals=0),
    )

    def placed(*arguments):
        return f(
            *[
                pltpu.with_memory_space_constraint(x, HBM) if space == HBM else x
                for x, space in zip(arguments, spaces)
            ]
        )

    return placed


def started(pairs, sems):
    copies = [pltpu.make_async_copy(src, dst, sems.at[n]) for n, (src, dst) in enumerate(pairs)]
    for copy in copies:
        copy.start()
    return copies


def shaped(dims, kind):
    return jax.ShapeDtypeStruct(dims, kind)


def across(columns):
    return jnp.sum(jnp.transpose(columns), axis=0, keepdims=True)


def down(row):
    return jnp.transpose(jnp.broadcast_to(row, (128, 128)))


def arrived(ref):
    parts = [jnp.sum(ref[16 * n : 16 * n + 16], axis=0) for n in range(16)]
    while len(parts) > 1:
        parts = [a + b for a, b in zip(parts[::2], parts[1::2])]
    return parts[0]


def shifted(slab, lane):
    before = jnp.where(lane == 0, 0.0, pltpu.roll(slab, 1, axis=1))
    after = jnp.where(lane == Z - 1, 0.0, pltpu.roll(slab, Z - 1, axis=1))
    return jnp.concatenate([before, slab, after], 0)


def lanes():
    return lax.broadcasted_iota(jnp.int32, (C, Z), 1)


def spread_kernel(
    one_ref, two_ref, up_ref, vol_ref, c1_ref, c2_ref, ug_ref, vol3_out, down_ref, up_x_ref, stat_ref,
    held, vol3, sems, out_sem,
):
    sources = (("vol", vol_ref, None), ("c1", one_ref, c1_ref), ("c2", two_ref, c2_ref), ("ug", up_ref, ug_ref))
    copies = started([(src.at[0], held.at[n]) for n, (_, src, _) in enumerate(sources)], sems)
    lane = lanes()
    parts = []
    for n, (name, _, dst) in enumerate(sources):
        copies[n].wait()
        total, squares = jnp.zeros((C, Z), F32), jnp.zeros((C, Z), F32)
        for x in range(B):
            turned_x = jnp.swapaxes(held[n, :, x].astype(F32), 0, 1)
            for y in range(B):
                slab = turned_x[y]
                if name == "vol":
                    vol3[x, :, y * Z : (y + 1) * Z] = shifted(slab, lane).astype(BF16)
                    continue
                if name in ("c1", "c2"):
                    total, squares = total + slab, squares + slab * slab
                dst[x, :, y * Z : (y + 1) * Z] = slab.astype(BF16)
        if name == "vol":
            leaving = pltpu.make_async_copy(vol3, vol3_out, out_sem.at[0])
            leaving.start()
        if name in ("c1", "c2"):
            parts += [total, squares]
    own = {"c1": c1_ref, "c2": c2_ref, "ug": ug_ref}
    for side, ref in ((-1, down_ref), (1, up_x_ref)):
        for i, (f, x) in enumerate(layers_x(side)):
            ref[i] = own[f][x]
    row = across(jnp.concatenate(parts, 0))
    stat_ref[...] = jnp.broadcast_to(row[None], stat_ref.shape)
    leaving.wait()


def pack_kernel(c1_ref, c2_ref, ug_ref, low_ref, high_ref, down_ref, up_ref):
    where = {}
    for f, w, ref in (("c1", 1, c1_ref), ("c2", 2, c2_ref), ("ug", 2, ug_ref)):
        for x in range(B):
            where[(f, x + w)] = (ref, x)
    for side, ref in ((-1, low_ref), (1, high_ref)):
        for i, key in enumerate(places_x(side)):
            where[key] = (ref, i)
    for side, out in ((-1, down_ref), (1, up_ref)):
        for i, (f, y, x) in enumerate(slabs_y(side)):
            ref, n = where[(f, x)]
            out[i] = ref[n, :, y * Z : (y + 1) * Z]


def extend_kernel(
    pos_ref, stat_ref, par_ref, c1_ref, c2_ref, slope_ref, xlow_ref, xhigh_ref, vol3_in, ylow_in, yhigh_in,
    c1x_out, c2x_out, slopex_out, turn_out, act3_out, r_out, r_ref, c1x, c2x, slopex, turn, act3, ugx, vol3, sems, out_sems,
):
    target = {"c1": c1x, "c2": c2x, "ug": ugx}
    pairs = []
    for side, ref in ((-1, ylow_in), (1, yhigh_in)):
        for first, count, f, y in places_y(side):
            pairs.append((ref.at[pl.ds(first, count)], target[f].at[:, :, pl.ds(y * Z, Z)]))
    pairs.append((vol3_in, vol3))
    arriving = started(pairs, sems)
    (mean1, inv1), (mean2, inv2) = norms(stat_ref)
    gain1, bias1, gain2, bias2 = par_ref[0:32], par_ref[32:64], par_ref[64:96], par_ref[96:128]
    lane = lanes()

    def activation(x, carry):
        for y in range(B):
            cut = slice(y * Z, (y + 1) * Z)
            cent = (c1_ref[x, :, cut].astype(F32) - mean1) * inv1
            pre = gain1 * cent + bias1
            s = sigmoid(pre)
            act3[x, :, cut] = shifted((pre * s).astype(BF16).astype(F32), lane).astype(BF16)
            turn[x + 1, :, (y + 1) * Z : (y + 2) * Z] = s * (1.0 + pre * (1.0 - s))
        return carry

    lax.fori_loop(0, B, activation, 0)
    leaving = started([(act3, act3_out)], out_sems)
    for f, w, own in (("c1", 1, c1_ref), ("c2", 2, c2_ref)):
        for x in range(B):
            target[f][x + w, :, w * Z : (w + B) * Z] = own[x]
    width = dict(FIELDS)
    for side, ref in ((-1, xlow_ref), (1, xhigh_ref)):
        for i, (f, x) in enumerate(places_x(side)):
            w = width[f]
            target[f][x, :, w * Z : (w + B) * Z] = ref[i]
    for copy in arriving:
        copy.wait()
    leaving += started([(c1x, c1x_out), (c2x, c2x_out)], out_sems.at[pl.ds(1, 2)])

    def slope_at(x, y):
        cut = slice(y * Z, (y + 1) * Z)
        cent = (c2x[x, :, cut].astype(F32) - mean2) * inv2
        slopex[x, :, cut] = ugx[x, :, cut].astype(F32) * silu_slope(gain2 * cent + bias2)

    def ends(i, carry):
        x = jnp.where(i < 2, i, i + B)
        for y in range(B + 4):
            slope_at(x, y)
        return carry

    lax.fori_loop(0, 4, ends, 0)

    def between(x, carry):
        for y in (0, 1, B + 2, B + 3):
            slope_at(x + 2, y)
        slopex[x + 2, :, 2 * Z : (2 + B) * Z] = slope_ref[x]
        return carry

    lax.fori_loop(0, B, between, 0)
    leaving += started([(slopex, slopex_out)], out_sems.at[pl.ds(3, 1)])

    def turn_at(x, y):
        cut = slice(y * Z, (y + 1) * Z)
        cent = (c1x[x, :, cut].astype(F32) - mean1) * inv1
        turn[x, :, cut] = silu_slope(gain1 * cent + bias1)

    for x in (0, B + 1):
        for y in range(B + 2):
            turn_at(x, y)

    def sides(x, carry):
        turn_at(x + 1, 0)
        turn_at(x + 1, B + 1)
        return carry

    lax.fori_loop(0, B, sides, 0)
    leaving += started([(turn, turn_out)], out_sems.at[pl.ds(4, 1)])

    sx, sy = pos_ref[0], pos_ref[1]
    row = lax.broadcasted_iota(jnp.int32, (16, B * Z), 0)
    gy = sy * B + lax.broadcasted_iota(jnp.int32, (16, B * Z), 1) // Z
    wy = gy + 1 - row % 3
    ok_y = (wy >= 0) & (wy < 4 * B) & (row < 9)

    def body(x, acc):
        wx = sx * B + x + 1 - row // 3
        inside = jnp.where(ok_y & (wx >= 0) & (wx < 4 * B), 1.0, 0.0).astype(BF16)
        lhs = jnp.concatenate([windows(c1x, x, 2, 2, B), inside], 0)
        return acc + lax.dot_general(lhs, vol3[x], TRANSPOSED, preferred_element_type=F32)

    acc = lax.fori_loop(0, B, body, jnp.zeros((9 * C + 16, 3 * C), F32), unroll=2)
    r_ref[...] = turned(acc).astype(BF16)
    leaving += started([(r_ref, r_out)], out_sems.at[pl.ds(5, 1)])
    for copy in leaving:
        copy.wait()


TRANSPOSED = (((1,), (1,)), ((), ()))


def turned(acc):
    rows = acc.shape[0]
    full = jnp.concatenate([acc, jnp.zeros((384 - rows, 3 * C), F32)], 0)
    full = jnp.concatenate([full, jnp.zeros((384, 128 - 3 * C), F32)], 1)
    return jnp.concatenate([jnp.transpose(full[i * 128 : (i + 1) * 128]) for i in range(3)], 1)


def moments(total, squares):
    mean = total * (1.0 / CELLS)
    inv = lax.rsqrt(squares * (1.0 / CELLS) - mean * mean + EPS)
    return mean, inv


def norms(stat_ref):
    cols = down(stat_ref[0:1])
    return moments(cols[0:32], cols[32:64]), moments(cols[64:96], cols[96:128])


def sigmoid(v):
    return 0.5 * jnp.tanh(0.5 * v) + 0.5


def silu_slope(v):
    s = sigmoid(v)
    return s * (1.0 + v * (1.0 - s))


def sums_two_kernel(got_ref, par_ref, c2_ref, ug_ref, out_ref, row_ref, slope_ref):
    row = arrived(got_ref)
    row_ref[...] = jnp.broadcast_to(row, (8, 128))
    _, (mean2, inv2) = norms(row_ref)
    gain, bias = par_ref[64:96], par_ref[96:128]

    def body(x, acc):
        b, g = acc
        for y in range(B):
            cent = (c2_ref[x, :, y * Z : (y + 1) * Z].astype(F32) - mean2) * inv2
            up = ug_ref[x, :, y * Z : (y + 1) * Z].astype(F32)
            slope = up * silu_slope(gain * cent + bias)
            slope_ref[x, :, y * Z : (y + 1) * Z] = slope
            b, g = b + slope, g + slope * cent
        return b, g

    zero = jnp.zeros((C, Z), F32)
    b, g = lax.fori_loop(0, B, body, (zero, zero))
    out = across(jnp.concatenate([b, g, zero, zero], 0))
    out_ref[...] = jnp.broadcast_to(out[None], out_ref.shape)


def windows(ref, x, first, y_first, count):
    parts = []
    for kx in range(3):
        for ky in range(3):
            parts.append(ref[x + first - kx, :, (y_first - ky) * Z : (y_first - ky + count) * Z])
    return jnp.concatenate(parts, 0)


def unshift(t, y, lane):
    left = t[0:C, y * Z : (y + 1) * Z]
    mid = t[C : 2 * C, y * Z : (y + 1) * Z]
    right = t[2 * C : 3 * C, y * Z : (y + 1) * Z]
    out = mid + jnp.where(lane == Z - 1, 0.0, pltpu.roll(left, Z - 1, axis=1))
    return out + jnp.where(lane == 0, 0.0, pltpu.roll(right, 1, axis=1))


def as_matrix(src, dst):
    for kz in range(3):
        parts = [src[kx, ky, kz].astype(F32) for kx in range(3) for ky in range(3)]
        dst[kz * C : (kz + 1) * C, :] = jnp.concatenate(parts, 1).astype(BF16)


def three(value):
    hi = value.astype(BF16).astype(F32)
    mid = (value - hi).astype(BF16).astype(F32)
    lo = value - hi - mid
    return hi, mid, lo


MARKS = 96


def moved(row, lanes_up):
    return pltpu.roll(row, lanes_up, axis=1) if lanes_up else row


def sum_rows(sums):
    lane = lax.broadcasted_iota(jnp.int32, (1, 128), 1)
    hi, mid, lo = (jnp.where(lane < 64, part, 0.0) for part in three(sums))
    return hi + moved(mid, 64), lo


def sums_of(total):
    return total[21:22] + moved(total[21:22], 64) + total[22:23]


def middle_kernel(
    pos_ref, got_ref, stat_ref, par_ref, raw, c1x_in, c2x_in, slopex_in, turn_in, vol3_in, act3_in, r_in,
    msg_ref, slope_ref, row_ref, c1x_ref, w_ref, c2x_ref, slopex_ref, turn_ref, vol3_ref, act3_ref, r_ref,
    grad, sems, row_sems,
):
    cuts = [pl.ds(n * 3, 3) for n in range(4)]
    early = started(
        [(src.at[cut], dst.at[cut]) for cut in cuts for src, dst in ((slopex_in, slopex_ref), (c2x_in, c2x_ref))],
        row_sems,
    )
    arriving = started(
        [
            (turn_in, turn_ref),
            (c1x_in, c1x_ref),
            (vol3_in, vol3_ref),
            (act3_in, act3_ref),
            (r_in, r_ref),
        ],
        sems,
    )
    sx, sy = pos_ref[0], pos_ref[1]
    row = arrived(got_ref)
    row_ref[...] = jnp.broadcast_to(row, (8, 128))
    cols = down(row)
    (mean1, inv1), (mean2, inv2) = norms(stat_ref)
    amp = par_ref[64:96] * inv2
    by = amp * inv2 * cols[32:64] * (1.0 / CELLS)
    off = amp * cols[0:32] * (1.0 / CELLS) - by * mean2
    lane = lanes()
    inside_y = {
        y: jnp.where(sy > 0, 1.0, 0.0) if y < 2 else jnp.where(sy < 3, 1.0, 0.0)
        for y in (0, 1, B + 2, B + 3)
    }

    def first(x, carry):
        gx = sx * B + x - 2
        inside_x = jnp.where((gx >= 0) & (gx < 4 * B), 1.0, 0.0)
        for y in range(B + 4):
            cut = slice(y * Z, (y + 1) * Z)
            value = amp * slopex_ref[x, :, cut] - by * c2x_ref[x, :, cut].astype(F32) - off
            keep = inside_x * inside_y[y] if y in inside_y else inside_x
            grad[x, :, cut] = (value * keep).astype(BF16)
        return carry

    as_matrix(raw, w_ref)
    for n in range(4):
        early[2 * n].wait()
        early[2 * n + 1].wait()
        lax.fori_loop(3 * n, 3 * n + 3, first, 0)
    arriving[0].wait()
    arriving[1].wait()
    inside_y = {0: jnp.where(sy > 0, 1.0, 0.0), B + 1: jnp.where(sy < 3, 1.0, 0.0)}

    def second(x, acc):
        b, g = acc
        gx = sx * B + x - 1
        inside_x = jnp.where((gx >= 0) & (gx < 4 * B), 1.0, 0.0)
        own_x = jnp.where((x >= 1) & (x <= B), 1.0, 0.0)
        t = jnp.dot(w_ref[...], windows(grad, x, 2, 2, B + 2), preferred_element_type=F32)
        bx, gsum = jnp.zeros((C, Z), F32), jnp.zeros((C, Z), F32)
        for y in range(B + 2):
            cut = slice(y * Z, (y + 1) * Z)
            slope = unshift(t, y, lane) * turn_ref[x, :, cut]
            if 1 <= y <= B:
                bx, gsum = bx + slope, gsum + slope * c1x_ref[x, :, cut].astype(F32)
            inside = inside_x * inside_y[y] if y in inside_y else inside_x
            slope_ref[x, :, cut] = (slope * inside).astype(BF16)
        gsum = (gsum - mean1 * bx) * inv1
        return b + bx * own_x, g + gsum * own_x

    zero = jnp.zeros((C, Z), F32)
    b, g = lax.fori_loop(0, B + 2, second, (zero, zero), unroll=5)

    def third(x, acc):
        s, f = acc
        s = s + lax.dot_general(windows(slope_ref, x, 2, 2, B), vol3_ref[x], TRANSPOSED, preferred_element_type=F32)
        f = f + lax.dot_general(windows(grad, x, 3, 3, B), act3_ref[x], TRANSPOSED, preferred_element_type=F32)
        return s, f

    for copy in arriving[2:]:
        copy.wait()
    empty = jnp.zeros((9 * C, 3 * C), F32)
    s, f = lax.fori_loop(0, B, third, (empty, empty), unroll=4)
    sums = across(jnp.concatenate([b, g, zero, zero], 0))
    rows = []
    for marked, part in ((False, turned(s)), (True, r_ref[...].astype(F32)), (False, turned(f))):
        packed = zero
        for kz in range(3):
            band = part[kz * C : (kz + 1) * C]
            rows += [band[:, 0:128][None], band[:, 128:256][None]]
            end = band[:, 256:384]
            packed += moved(jnp.where(lane < C, end, 0.0), kz * C)
            if marked:
                packed += moved(jnp.where((lane >= C) & (lane < C + 9), end, 0.0), MARKS - C + 9 * kz)
        rows.append(packed[None])
    rows += [jnp.broadcast_to(part, (C, 128))[None] for part in sum_rows(sums)] + [zero[None]]
    for n in range(3):
        block = jnp.swapaxes(jnp.concatenate(rows[8 * n : 8 * n + 8], 0), 0, 1)
        msg_ref[:, 8 * n : 8 * n + 8, :] = block.astype(BF16)


def relay_kernel(got_ref, out_ref):
    total = jnp.sum(got_ref[...].astype(F32), axis=0)
    first, second = sum_rows(sums_of(total))
    out = jnp.concatenate([total[0:21], first, second, total[23:24]], 0).astype(BF16)
    out_ref[...] = jnp.broadcast_to(out[None], out_ref.shape)


def share_kernel(got_ref, stat_ref, lanepar_ref, out_ref, row_ref):
    total = jnp.sum(got_ref[...].astype(F32), axis=0)
    sums = sums_of(total)
    row_ref[...] = jnp.broadcast_to(sums, (8, 128))
    lane = lax.broadcasted_iota(jnp.int32, (1, 128), 1)
    stat = stat_ref[0:1]
    mean = stat * (1.0 / CELLS)
    squares = pltpu.roll(stat, 96, axis=1) * (1.0 / CELLS)
    inv = lax.rsqrt(jnp.where(lane < C, squares - mean * mean, 0.0) + EPS)
    g = pltpu.roll(sums, 96, axis=1)
    alpha = lanepar_ref[0:1] * inv
    gamma = alpha * inv * g * (1.0 / CELLS)
    delta = alpha * sums * (1.0 / CELLS) - gamma * mean
    rows = jnp.where(lane < C, jnp.concatenate([alpha, gamma, delta], 0), 0.0)
    rows = jnp.concatenate([rows, jnp.zeros((5, 128), F32)], 0)
    a = lax.broadcasted_iota(jnp.int32, (128, 896), 0)
    o = lax.broadcasted_iota(jnp.int32, (128, 896), 1)
    tile = jnp.where(o[:, 0:128] % C == a[:, 0:128], 1.0, 0.0)
    wide = jnp.dot(rows, tile, precision=lax.Precision.HIGHEST, preferred_element_type=F32)
    row = o // 128
    block = (o % 128) // C
    mark = jnp.where(row < 6, MARKS + 9 * (row // 2) + 4 * (row % 2) + block, MARKS + 9 * block + 8)
    spread = jnp.where((mark == a) & ((row < 6) | (block < 3)), 1.0, 0.0)
    marks = jnp.concatenate([total[13:14], jnp.zeros((7, 128), F32)], 0)
    ones = jnp.dot(marks, spread, precision=lax.Precision.HIGHEST, preferred_element_type=F32)
    parts = []
    for r in range(7):
        parts.append(
            wide[0:1] * total[r : r + 1]
            - wide[1:2] * total[7 + r : 8 + r]
            - wide[2:3] * ones[0:1, r * 128 : (r + 1) * 128]
        )
    out = jnp.concatenate(parts + [total[14:21], jnp.zeros((2, 128), F32)], 0) * SCALE
    out_ref[...] = jnp.broadcast_to(out.astype(BF16)[None], out_ref.shape)


def last_kernel(
    mask_ref, sum_ref, two_ref, stat_ref, par_ref, slope_ref, c1x_ref, raw,
    out_ref, gain1_ref, bias1_ref, gain2_ref, bias2_ref, grad, done, w_ref, out_sems,
):
    for ref, bias_ref, gain_ref in ((sum_ref, bias1_ref, gain1_ref), (two_ref, bias2_ref, gain2_ref)):
        scaled = ref[0:1] * SCALE
        bias_ref[...] = scaled[:, 0:C]
        gain_ref[...] = pltpu.roll(scaled, 96, axis=1)[:, 0:C]
    cols = down(sum_ref[0:1])
    (mean, inv), _ = norms(stat_ref)
    b, g = cols[0:32] * (1.0 / CELLS), cols[32:64] * (1.0 / CELLS)
    amp = par_ref[0:32] * inv
    by = amp * inv * g
    off = amp * b - by * mean
    lane = lanes()
    sx, sy = mask_ref[0], mask_ref[1]
    inside_y = {0: jnp.where(sy > 0, 1.0, 0.0), B + 1: jnp.where(sy < 3, 1.0, 0.0)}

    def first(x, carry):
        gx = sx * B + x - 1
        inside_x = jnp.where((gx >= 0) & (gx < 4 * B), 1.0, 0.0)
        for y in range(B + 2):
            cut = slice(y * Z, (y + 1) * Z)
            value = amp * slope_ref[x, :, cut].astype(F32) - by * c1x_ref[x, :, cut].astype(F32) - off
            keep = inside_x * inside_y[y] if y in inside_y else inside_x
            grad[x, :, cut] = (value * keep).astype(BF16)
        return carry

    as_matrix(raw, w_ref)
    lax.fori_loop(0, B + 2, first, 0)

    leaving = []
    for x in range(B):
        t = jnp.dot(w_ref[...], windows(grad, x, 2, 2, B), preferred_element_type=F32)
        rows = jnp.concatenate([unshift(t, y, lane)[None] for y in range(B)], 0)
        done[x] = jnp.swapaxes(rows, 0, 1).astype(BF16)
        leaving.append(pltpu.make_async_copy(done.at[x], out_ref.at[0, :, x], out_sems.at[x]))
        leaving[-1].start()
    for copy in leaving:
        copy.wait()


def filters_kernel(got_ref, one_ref, two_ref):
    rows = jnp.swapaxes(got_ref[...].astype(F32), 0, 1)
    for m, ref in enumerate((one_ref, two_ref)):
        for kz in range(3):
            for k in range(9):
                if k < 8:
                    slab, i = rows[m * 7 + kz * 2 + k // 4], k % 4
                else:
                    slab, i = rows[m * 7 + 6], kz
                ref[k // 3, k % 3, kz] = slab[:, i * C : (i + 1) * C]


def exchanged(array, axes):
    return lax.all_to_all(array, axes, 0, 0, tiled=True)


def per_device(
    volume, conv_one, conv_two, upper_grad, weight_one, weight_two, gain_one, bias_one, gain_two, bias_two
):
    pos = jnp.stack([lax.axis_index("sx"), lax.axis_index("sy")]).astype(jnp.int32)
    packed = jnp.concatenate([gain_one, bias_one, gain_two, bias_two])
    par = jnp.broadcast_to(packed[:, None], (128, 128))
    lanepar = jnp.broadcast_to(packed[None, :], (8, 128))
    everyone = shaped((256, 1, 128), F32)
    block = shaped((B, C, B * Z), BF16)
    three_fold = shaped((B, 3 * C, B * Z), BF16)
    near = shaped((B + 2, C, (B + 2) * Z), BF16)
    far = shaped((B + 4, C, (B + 4) * Z), BF16)
    near_wide, far_wide, block_wide = (shaped(a.shape, F32) for a in (near, far, block))
    row = shaped((8, 128), F32)

    def room(like):
        return pltpu.VMEM(like.shape, like.dtype)

    def sems(count):
        return pltpu.SemaphoreType.DMA((count,))

    along_x = shaped((len(layers_x(1)), C, B * Z), BF16)
    c1, c2, ug, vol3, send_down, send_up, stats = call(
        spread_kernel,
        [block, block, block, three_fold, along_x, along_x, everyone],
        scratch=[
            pltpu.VMEM((4, C, B, B, Z), BF16),
            room(three_fold),
            sems(4),
            sems(1),
        ],
        spaces=[HBM] * 4,
        homes=[VMEM] * 3 + [HBM] + [VMEM] * 3,
        limit=10,
    )(conv_one, conv_two, upper_grad, volume)
    up = [(i, i + 1) for i in range(3)]
    down_ = [(i + 1, i) for i in range(3)]
    x_low = lax.ppermute(send_up, "sx", up)
    x_high = lax.ppermute(send_down, "sx", down_)
    got_stats = exchanged(stats, ALL)
    along_y = shaped((len(slabs_y(1)), C, Z), BF16)
    send_down, send_up = call(pack_kernel, [along_y, along_y], spaces=[VMEM] * 5)(c1, c2, ug, x_low, x_high)
    y_low = lax.ppermute(send_up, "sy", up)
    y_high = lax.ppermute(send_down, "sy", down_)

    sums_two, stat_row, slope_two = call(
        sums_two_kernel, [everyone, row, block_wide], spaces=[VMEM] * 4
    )(got_stats, par, c2, ug)
    got_two = exchanged(sums_two, ALL)
    r_shape = shaped((128, 384), BF16)
    c1x, c2x, slopex, turn, act3, r = call(
        extend_kernel,
        [near, far, far_wide, near_wide, three_fold, r_shape],
        scratch=[
            room(r_shape), room(near), room(far), room(far_wide), room(near_wide), room(three_fold), room(far), room(three_fold), sems(11), sems(6)
        ],
        flops=5 * 10**9,
        spaces=[SMEM] + [VMEM] * 7 + [HBM] * 3,
        homes=[HBM] * 6,
        limit=16,
    )(pos, stat_row, par, c1, c2, slope_two, x_low, x_high, vol3, y_low, y_high)

    terms, slope, row_two, c1x_own = call(
        middle_kernel,
        [shaped((32, 24, 128), BF16), near, row, near],
        scratch=[
            pltpu.VMEM((3 * C, 9 * C), BF16), room(far), room(far_wide), room(near_wide), room(three_fold),
            room(three_fold), room(r_shape), room(far), sems(5), sems(8),
        ],
        flops=4 * 10**9,
        spaces=[SMEM] + [VMEM] * 4 + [HBM] * 7,
        limit=18,
    )(pos, got_two, stat_row, par, weight_two, c1x, c2x, slopex, turn, vol3, act3, r)

    got_terms = exchanged(terms, PLANE)
    relay = call(relay_kernel, shaped((8, 24, 128), BF16), spaces=[VMEM])(got_terms)
    got_relay = exchanged(relay, "dp_0")
    shares, row_one = call(
        share_kernel, [shaped((32, 16, 128), BF16), row], spaces=[VMEM] * 3
    )(got_relay, stat_row, lanepar)
    got_shares = exchanged(shares, PLANE)
    vector = shaped((1, C), F32)
    input_grad, gain_one_grad, bias_one_grad, gain_two_grad, bias_two_grad = call(
        last_kernel,
        [shaped((1, C, B, B, Z), BF16), vector, vector, vector, vector],
        scratch=[
            room(near), pltpu.VMEM((B, C, B, Z), BF16), pltpu.VMEM((3 * C, 9 * C), BF16), sems(8)
        ],
        flops=4 * 10**9,
        spaces=[SMEM] + [VMEM] * 7,
        homes=[HBM] + [VMEM] * 4,
        limit=10,
    )(pos, row_one, row_two, stat_row, par, slope, c1x_own, weight_one)
    filters = shaped((3, 3, 3, C, C), F32)
    filter_one, filter_two = call(
        filters_kernel, [filters, filters], spaces=[VMEM]
    )(got_shares)
    return (
        input_grad, filter_one, filter_two, gain_one_grad[0], bias_one_grad[0], gain_two_grad[0], bias_two_grad[0]
    )


def solution(mesh):
    finer = Mesh(
        mesh.devices.reshape(8, 2, mesh.shape["sx"], mesh.shape["sy"]), ("dp_0", "dp_1", "sx", "sy")
    )
    field = P(DP, None, "sx", "sy", None)
    return jax.shard_map(
        per_device,
        mesh=finer,
        in_specs=(field,) * 4 + (P(),) * 6,
        out_specs=(field,) + (P(),) * 6,
        check_vma=False,
    )
```

```python
import math

import jax
import jax.numpy as jnp
from jax import lax
from jax.experimental import pallas as pl
from jax.experimental.pallas import tpu as pltpu
from jax.sharding import Mesh
from jax.sharding import PartitionSpec as P

DP = ("dp_0", "dp_1")
ALL = ("dp_0", "dp_1", "sx", "sy")
PLANE = ("dp_1", "sx", "sy")
EPS = 1e-05
F32 = jnp.float32
BF16 = jnp.bfloat16
C = 32
B = 8
Z = 128
CELLS = float(16 * 32 * 32 * Z)
SCALE = 1.0 / math.sqrt(CELLS)

VMEM = pltpu.MemorySpace.VMEM
SMEM = pltpu.MemorySpace.SMEM
HBM = pltpu.MemorySpace.HBM
FIELDS = (("c2", 2), ("ug", 2), ("c1", 1))


def span(side, width):
    return range(B - width, B) if side > 0 else range(width)


def landing(side, width):
    return range(B + width, B + 2 * width) if side > 0 else range(width)


def layers_x(side):
    return [(f, x) for f, w in FIELDS for x in span(side, w)]


def places_x(side):
    return [(f, x) for f, w in FIELDS for x in landing(side, w)]


def slabs_y(side):
    return [(f, y, x) for f, w in FIELDS for y in span(side, w) for x in range(B + 2 * w)]


def places_y(side):
    runs, first = [], 0
    for f, w in FIELDS:
        for y in landing(side, w):
            runs.append((first, B + 2 * w, f, y))
            first += B + 2 * w
    return runs


def call(kernel, outs, scratch=(), flops=0, spaces=(), limit=6, homes=None):
    single = not isinstance(outs, (list, tuple))
    shapes = [outs] if single else list(outs)
    homes = homes or [VMEM] * len(shapes)
    specs = [pl.BlockSpec(memory_space=space) for space in homes]
    shapes = [HBM(x.shape, x.dtype) if home == HBM else x for x, home in zip(shapes, homes)]
    f = pl.pallas_call(
        kernel,
        out_shape=shapes[0] if single else tuple(shapes),
        in_specs=[pl.BlockSpec(memory_space=space) for space in spaces],
        out_specs=specs[0] if single else tuple(specs),
        scratch_shapes=list(scratch),
        compiler_params=pltpu.CompilerParams(vmem_limit_bytes=limit * 2**20),
        cost_estimate=pl.CostEstimate(flops=flops, bytes_accessed=1 << 20, transcendentals=0),
    )

    def placed(*arguments):
        return f(
            *[
                pltpu.with_memory_space_constraint(x, HBM) if space == HBM else x
                for x, space in zip(arguments, spaces)
            ]
        )

    return placed


def started(pairs, sems):
    copies = [pltpu.make_async_copy(src, dst, sems.at[n]) for n, (src, dst) in enumerate(pairs)]
    for copy in copies:
        copy.start()
    return copies


def shaped(dims, kind):
    return jax.ShapeDtypeStruct(dims, kind)


def across(columns):
    return jnp.sum(jnp.transpose(columns), axis=0, keepdims=True)


def down(row):
    return jnp.transpose(jnp.broadcast_to(row, (128, 128)))


def arrived(ref):
    parts = [jnp.sum(ref[16 * n : 16 * n + 16], axis=0) for n in range(16)]
    while len(parts) > 1:
        parts = [a + b for a, b in zip(parts[::2], parts[1::2])]
    return parts[0]


def shifted(slab, lane):
    before = jnp.where(lane == 0, 0.0, pltpu.roll(slab, 1, axis=1))
    after = jnp.where(lane == Z - 1, 0.0, pltpu.roll(slab, Z - 1, axis=1))
    return jnp.concatenate([before, slab, after], 0)


def lanes():
    return lax.broadcasted_iota(jnp.int32, (C, Z), 1)


def spread_kernel(
    one_ref, two_ref, up_ref, vol_ref, c1_ref, c2_ref, ug_ref, vol3_out, down_ref, up_x_ref, stat_ref,
    held, vol3, sems, out_sem,
):
    sources = (("vol", vol_ref, None), ("c1", one_ref, c1_ref), ("c2", two_ref, c2_ref), ("ug", up_ref, ug_ref))
    copies = started([(src.at[0], held.at[n]) for n, (_, src, _) in enumerate(sources)], sems)
    lane = lanes()
    parts = []
    for n, (name, _, dst) in enumerate(sources):
        copies[n].wait()
        total, squares = jnp.zeros((C, Z), F32), jnp.zeros((C, Z), F32)
        for x in range(B):
            turned_x = jnp.swapaxes(held[n, :, x].astype(F32), 0, 1)
            for y in range(B):
                slab = turned_x[y]
                if name == "vol":
                    vol3[x, :, y * Z : (y + 1) * Z] = shifted(slab, lane).astype(BF16)
                    continue
                if name in ("c1", "c2"):
                    total, squares = total + slab, squares + slab * slab
                dst[x, :, y * Z : (y + 1) * Z] = slab.astype(BF16)
        if name == "vol":
            leaving = pltpu.make_async_copy(vol3, vol3_out, out_sem.at[0])
            leaving.start()
        if name in ("c1", "c2"):
            parts += [total, squares]
    own = {"c1": c1_ref, "c2": c2_ref, "ug": ug_ref}
    for side, ref in ((-1, down_ref), (1, up_x_ref)):
        for i, (f, x) in enumerate(layers_x(side)):
            ref[i] = own[f][x]
    row = across(jnp.concatenate(parts, 0))
    stat_ref[...] = jnp.broadcast_to(row[None], stat_ref.shape)
    leaving.wait()


def pack_kernel(c1_ref, c2_ref, ug_ref, low_ref, high_ref, down_ref, up_ref):
    where = {}
    for f, w, ref in (("c1", 1, c1_ref), ("c2", 2, c2_ref), ("ug", 2, ug_ref)):
        for x in range(B):
            where[(f, x + w)] = (ref, x)
    for side, ref in ((-1, low_ref), (1, high_ref)):
        for i, key in enumerate(places_x(side)):
            where[key] = (ref, i)
    for side, out in ((-1, down_ref), (1, up_ref)):
        for i, (f, y, x) in enumerate(slabs_y(side)):
            ref, n = where[(f, x)]
            out[i] = ref[n, :, y * Z : (y + 1) * Z]


def extend_kernel(
    pos_ref, stat_ref, par_ref, c1_ref, xlow_ref, xhigh_ref, vol3_in, ylow_in, yhigh_in,
    c1x_out, c2x_out, slopex_out, turn_out, act3_out, r_out, r_ref, c1x, c2x, slopex, turn, act3, ugx, vol3, sems, out_sems,
):
    target = {"c1": c1x, "c2": c2x, "ug": ugx}
    pairs = []
    for side, ref in ((-1, ylow_in), (1, yhigh_in)):
        for first, count, f, y in places_y(side):
            pairs.append((ref.at[pl.ds(first, count)], target[f].at[:, :, pl.ds(y * Z, Z)]))
    pairs.append((vol3_in, vol3))
    arriving = started(pairs, sems)
    (mean1, inv1), (mean2, inv2) = norms(stat_ref)
    gain1, bias1, gain2, bias2 = par_ref[0:32], par_ref[32:64], par_ref[64:96], par_ref[96:128]
    lane = lanes()

    def activation(x, carry):
        for y in range(B):
            cut = slice(y * Z, (y + 1) * Z)
            cent = (c1_ref[x, :, cut].astype(F32) - mean1) * inv1
            pre = gain1 * cent + bias1
            s = sigmoid(pre)
            act3[x, :, cut] = shifted((pre * s).astype(BF16).astype(F32), lane).astype(BF16)
            turn[x + 1, :, (y + 1) * Z : (y + 2) * Z] = s * (1.0 + pre * (1.0 - s))
        return carry

    lax.fori_loop(0, B, activation, 0)
    leaving = started([(act3, act3_out)], out_sems)
    for x in range(B):
        c1x[x + 1, :, Z : (1 + B) * Z] = c1_ref[x]
    width = dict(FIELDS)
    for side, ref in ((-1, xlow_ref), (1, xhigh_ref)):
        for i, (f, x) in enumerate(places_x(side)):
            w = width[f]
            target[f][x, :, w * Z : (w + B) * Z] = ref[i]
    for copy in arriving[:-1]:
        copy.wait()
    leaving += started([(c1x, c1x_out)] + [(c2x.at[cut], c2x_out.at[cut]) for cut in RIM], out_sems.at[pl.ds(1, 5)])

    def slope_at(x, y):
        cut = slice(y * Z, (y + 1) * Z)
        cent = (c2x[x, :, cut].astype(F32) - mean2) * inv2
        slopex[x, :, cut] = ugx[x, :, cut].astype(F32) * silu_slope(gain2 * cent + bias2)

    def ends(i, carry):
        x = jnp.where(i < 2, i, i + B)
        for y in range(B + 4):
            slope_at(x, y)
        return carry

    lax.fori_loop(0, 4, ends, 0)

    def between(x, carry):
        for y in (0, 1, B + 2, B + 3):
            slope_at(x + 2, y)
        return carry

    lax.fori_loop(0, B, between, 0)
    leaving += started([(slopex.at[cut], slopex_out.at[cut]) for cut in RIM], out_sems.at[pl.ds(6, 4)])

    def turn_at(x, y):
        cut = slice(y * Z, (y + 1) * Z)
        cent = (c1x[x, :, cut].astype(F32) - mean1) * inv1
        turn[x, :, cut] = silu_slope(gain1 * cent + bias1)

    for x in (0, B + 1):
        for y in range(B + 2):
            turn_at(x, y)

    def sides(x, carry):
        turn_at(x + 1, 0)
        turn_at(x + 1, B + 1)
        return carry

    lax.fori_loop(0, B, sides, 0)
    leaving += started([(turn, turn_out)], out_sems.at[pl.ds(10, 1)])

    sx, sy = pos_ref[0], pos_ref[1]
    row = lax.broadcasted_iota(jnp.int32, (16, B * Z), 0)
    gy = sy * B + lax.broadcasted_iota(jnp.int32, (16, B * Z), 1) // Z
    wy = gy + 1 - row % 3
    ok_y = (wy >= 0) & (wy < 4 * B) & (row < 9)

    def body(x, acc):
        wx = sx * B + x + 1 - row // 3
        inside = jnp.where(ok_y & (wx >= 0) & (wx < 4 * B), 1.0, 0.0).astype(BF16)
        lhs = jnp.concatenate([windows(c1x, x, 2, 2, B), inside], 0)
        return acc + lax.dot_general(lhs, vol3[x], TRANSPOSED, preferred_element_type=F32)

    arriving[-1].wait()
    acc = lax.fori_loop(0, B, body, jnp.zeros((9 * C + 16, 3 * C), F32), unroll=2)
    r_ref[...] = turned(acc).astype(BF16)
    leaving += started([(r_ref, r_out)], out_sems.at[pl.ds(11, 1)])
    for copy in leaving:
        copy.wait()


RIM = (
    (pl.ds(0, 2),),
    (pl.ds(B + 2, 2),),
    (pl.ds(2, B), slice(None), pl.ds(0, 2 * Z)),
    (pl.ds(2, B), slice(None), pl.ds((B + 2) * Z, 2 * Z)),
)

TRANSPOSED = (((1,), (1,)), ((), ()))


def turned(acc):
    rows = acc.shape[0]
    full = jnp.concatenate([acc, jnp.zeros((384 - rows, 3 * C), F32)], 0)
    full = jnp.concatenate([full, jnp.zeros((384, 128 - 3 * C), F32)], 1)
    return jnp.concatenate([jnp.transpose(full[i * 128 : (i + 1) * 128]) for i in range(3)], 1)


def moments(total, squares):
    mean = total * (1.0 / CELLS)
    inv = lax.rsqrt(squares * (1.0 / CELLS) - mean * mean + EPS)
    return mean, inv


def norms(stat_ref):
    cols = down(stat_ref[0:1])
    return moments(cols[0:32], cols[32:64]), moments(cols[64:96], cols[96:128])


def sigmoid(v):
    return 0.5 * jnp.tanh(0.5 * v) + 0.5


def silu_slope(v):
    s = sigmoid(v)
    return s * (1.0 + v * (1.0 - s))


def sums_two_kernel(got_ref, par_ref, c2_ref, ug_ref, out_ref, row_ref, slope_ref):
    row = arrived(got_ref)
    row_ref[...] = jnp.broadcast_to(row, (8, 128))
    _, (mean2, inv2) = norms(row_ref)
    gain, bias = par_ref[64:96], par_ref[96:128]

    def body(x, acc):
        b, g = acc
        for y in range(B):
            cent = (c2_ref[x, :, y * Z : (y + 1) * Z].astype(F32) - mean2) * inv2
            up = ug_ref[x, :, y * Z : (y + 1) * Z].astype(F32)
            slope = up * silu_slope(gain * cent + bias)
            slope_ref[x, :, y * Z : (y + 1) * Z] = slope
            b, g = b + slope, g + slope * cent
        return b, g

    zero = jnp.zeros((C, Z), F32)
    b, g = lax.fori_loop(0, B, body, (zero, zero))
    out = across(jnp.concatenate([b, g, zero, zero], 0))
    out_ref[...] = jnp.broadcast_to(out[None], out_ref.shape)


def windows(ref, x, first, y_first, count):
    parts = []
    for kx in range(3):
        for ky in range(3):
            parts.append(ref[x + first - kx, :, (y_first - ky) * Z : (y_first - ky + count) * Z])
    return jnp.concatenate(parts, 0)


def unshift(t, y, lane):
    left = t[0:C, y * Z : (y + 1) * Z]
    mid = t[C : 2 * C, y * Z : (y + 1) * Z]
    right = t[2 * C : 3 * C, y * Z : (y + 1) * Z]
    out = mid + jnp.where(lane == Z - 1, 0.0, pltpu.roll(left, Z - 1, axis=1))
    return out + jnp.where(lane == 0, 0.0, pltpu.roll(right, 1, axis=1))


def as_matrix(src, dst):
    for kz in range(3):
        parts = [src[kx, ky, kz].astype(F32) for kx in range(3) for ky in range(3)]
        dst[kz * C : (kz + 1) * C, :] = jnp.concatenate(parts, 1).astype(BF16)


def three(value):
    hi = value.astype(BF16).astype(F32)
    mid = (value - hi).astype(BF16).astype(F32)
    lo = value - hi - mid
    return hi, mid, lo


MARKS = 96


def moved(row, lanes_up):
    return pltpu.roll(row, lanes_up, axis=1) if lanes_up else row


def sum_rows(sums):
    lane = lax.broadcasted_iota(jnp.int32, (1, 128), 1)
    hi, mid, lo = (jnp.where(lane < 64, part, 0.0) for part in three(sums))
    return hi + moved(mid, 64), lo


def sums_of(total):
    return total[21:22] + moved(total[21:22], 64) + total[22:23]


def middle_kernel(
    pos_ref, got_ref, stat_ref, par_ref, raw, c2_ref, slope_two_ref, c1x_in, c2x_in, slopex_in, turn_in, vol3_in, act3_in, r_in,
    msg_ref, slope_ref, row_ref, w_ref, c1x_ref, c2x_ref, slopex_ref, turn_ref, vol3_ref, act3_ref, r_ref,
    grad, sems, row_sems,
):
    early = started(
        [(src.at[cut], dst.at[cut]) for cut in RIM for src, dst in ((slopex_in, slopex_ref), (c2x_in, c2x_ref))],
        row_sems,
    )
    arriving = started(
        [
            (turn_in, turn_ref),
            (c1x_in, c1x_ref),
            (vol3_in, vol3_ref),
            (act3_in, act3_ref),
            (r_in, r_ref),
        ],
        sems,
    )
    sx, sy = pos_ref[0], pos_ref[1]
    row = arrived(got_ref)
    row_ref[...] = jnp.broadcast_to(row, (8, 128))
    cols = down(row)
    (mean1, inv1), (mean2, inv2) = norms(stat_ref)
    amp = par_ref[64:96] * inv2
    by = amp * inv2 * cols[32:64] * (1.0 / CELLS)
    off = amp * cols[0:32] * (1.0 / CELLS) - by * mean2
    lane = lanes()
    inside_y = {
        y: jnp.where(sy > 0, 1.0, 0.0) if y < 2 else jnp.where(sy < 3, 1.0, 0.0)
        for y in (0, 1, B + 2, B + 3)
    }

    def own(x, carry):
        for y in range(B):
            cut = slice(y * Z, (y + 1) * Z)
            value = amp * slope_two_ref[x, :, cut] - by * c2_ref[x, :, cut].astype(F32) - off
            grad[x + 2, :, (y + 2) * Z : (y + 3) * Z] = value.astype(BF16)
        return carry

    lax.fori_loop(0, B, own, 0, unroll=2)
    as_matrix(raw, w_ref)

    def rim_at(x, y, inside_x):
        cut = slice(y * Z, (y + 1) * Z)
        value = amp * slopex_ref[x, :, cut] - by * c2x_ref[x, :, cut].astype(F32) - off
        keep = inside_x * inside_y[y] if y in inside_y else inside_x
        grad[x, :, cut] = (value * keep).astype(BF16)

    for copy in early[:4]:
        copy.wait()

    def ends(i, carry):
        x = jnp.where(i < 2, i, i + B)
        gx = sx * B + x - 2
        inside_x = jnp.where((gx >= 0) & (gx < 4 * B), 1.0, 0.0)
        for y in range(B + 4):
            rim_at(x, y, inside_x)
        return carry

    lax.fori_loop(0, 4, ends, 0)
    for copy in early[4:]:
        copy.wait()

    def sides(x, carry):
        for y in (0, 1, B + 2, B + 3):
            rim_at(x + 2, y, 1.0)
        return carry

    lax.fori_loop(0, B, sides, 0)
    arriving[0].wait()
    arriving[1].wait()
    inside_y = {0: jnp.where(sy > 0, 1.0, 0.0), B + 1: jnp.where(sy < 3, 1.0, 0.0)}

    def second(x, acc):
        b, g = acc
        gx = sx * B + x - 1
        inside_x = jnp.where((gx >= 0) & (gx < 4 * B), 1.0, 0.0)
        own_x = jnp.where((x >= 1) & (x <= B), 1.0, 0.0)
        t = jnp.dot(w_ref[...], windows(grad, x, 2, 2, B + 2), preferred_element_type=F32)
        bx, gsum = jnp.zeros((C, Z), F32), jnp.zeros((C, Z), F32)
        for y in range(B + 2):
            cut = slice(y * Z, (y + 1) * Z)
            slope = unshift(t, y, lane) * turn_ref[x, :, cut]
            if 1 <= y <= B:
                bx, gsum = bx + slope, gsum + slope * c1x_ref[x, :, cut].astype(F32)
            inside = inside_x * inside_y[y] if y in inside_y else inside_x
            slope_ref[x, :, cut] = (slope * inside).astype(BF16)
        gsum = (gsum - mean1 * bx) * inv1
        return b + bx * own_x, g + gsum * own_x

    zero = jnp.zeros((C, Z), F32)
    b, g = lax.fori_loop(0, B + 2, second, (zero, zero), unroll=5)

    def third(x, acc):
        s, f = acc
        s = s + lax.dot_general(windows(slope_ref, x, 2, 2, B), vol3_ref[x], TRANSPOSED, preferred_element_type=F32)
        f = f + lax.dot_general(windows(grad, x, 3, 3, B), act3_ref[x], TRANSPOSED, preferred_element_type=F32)
        return s, f

    for copy in arriving[2:]:
        copy.wait()
    empty = jnp.zeros((9 * C, 3 * C), F32)
    s, f = lax.fori_loop(0, B, third, (empty, empty), unroll=4)
    sums = across(jnp.concatenate([b, g, zero, zero], 0))
    rows = []
    for marked, part in ((False, turned(s)), (True, r_ref[...].astype(F32)), (False, turned(f))):
        packed = zero
        for kz in range(3):
            band = part[kz * C : (kz + 1) * C]
            rows += [band[:, 0:128][None], band[:, 128:256][None]]
            end = band[:, 256:384]
            packed += moved(jnp.where(lane < C, end, 0.0), kz * C)
            if marked:
                packed += moved(jnp.where((lane >= C) & (lane < C + 9), end, 0.0), MARKS - C + 9 * kz)
        rows.append(packed[None])
    rows += [jnp.broadcast_to(part, (C, 128))[None] for part in sum_rows(sums)] + [zero[None]]
    for n in range(3):
        block = jnp.swapaxes(jnp.concatenate(rows[8 * n : 8 * n + 8], 0), 0, 1)
        msg_ref[:, 8 * n : 8 * n + 8, :] = block.astype(BF16)


def relay_kernel(got_ref, out_ref):
    total = jnp.sum(got_ref[...].astype(F32), axis=0)
    first, second = sum_rows(sums_of(total))
    out = jnp.concatenate([total[0:21], first, second, total[23:24]], 0).astype(BF16)
    out_ref[...] = jnp.broadcast_to(out[None], out_ref.shape)


def selected(rows, choice):
    parts = jnp.concatenate(three(rows), 0).astype(BF16)
    out = jnp.dot(parts, choice.astype(BF16), preferred_element_type=F32)
    return out[0:8] + out[8:16] + out[16:24]


def share_kernel(got_ref, stat_ref, lanepar_ref, out_ref, row_ref):
    total = jnp.sum(got_ref[...].astype(F32), axis=0)
    sums = sums_of(total)
    row_ref[...] = jnp.broadcast_to(sums, (8, 128))
    lane = lax.broadcasted_iota(jnp.int32, (1, 128), 1)
    stat = stat_ref[0:1]
    mean = stat * (1.0 / CELLS)
    squares = pltpu.roll(stat, 96, axis=1) * (1.0 / CELLS)
    inv = lax.rsqrt(jnp.where(lane < C, squares - mean * mean, 0.0) + EPS)
    g = pltpu.roll(sums, 96, axis=1)
    alpha = lanepar_ref[0:1] * inv
    gamma = alpha * inv * g * (1.0 / CELLS)
    delta = alpha * sums * (1.0 / CELLS) - gamma * mean
    rows = jnp.where(lane < C, jnp.concatenate([alpha, gamma, delta], 0), 0.0)
    rows = jnp.concatenate([rows, jnp.zeros((5, 128), F32)], 0)
    a = lax.broadcasted_iota(jnp.int32, (128, 896), 0)
    o = lax.broadcasted_iota(jnp.int32, (128, 896), 1)
    tile = jnp.where(o[:, 0:128] % C == a[:, 0:128], 1.0, 0.0)
    wide = selected(rows, tile)
    row = o // 128
    block = (o % 128) // C
    mark = jnp.where(row < 6, MARKS + 9 * (row // 2) + 4 * (row % 2) + block, MARKS + 9 * block + 8)
    spread = jnp.where((mark == a) & ((row < 6) | (block < 3)), 1.0, 0.0)
    marks = jnp.concatenate([total[13:14], jnp.zeros((7, 128), F32)], 0)
    ones = selected(marks, spread)
    parts = []
    for r in range(7):
        parts.append(
            wide[0:1] * total[r : r + 1]
            - wide[1:2] * total[7 + r : 8 + r]
            - wide[2:3] * ones[0:1, r * 128 : (r + 1) * 128]
        )
    out = jnp.concatenate(parts + [total[14:21], jnp.zeros((2, 128), F32)], 0) * SCALE
    out_ref[...] = jnp.broadcast_to(out.astype(BF16)[None], out_ref.shape)


def last_kernel(
    mask_ref, sum_ref, two_ref, stat_ref, par_ref, slope_ref, raw, c1x_in,
    out_ref, gain1_ref, bias1_ref, gain2_ref, bias2_ref, grad, done, w_ref, c1x_ref, out_sems, sems,
):
    arriving = started([(c1x_in, c1x_ref)], sems)
    for ref, bias_ref, gain_ref in ((sum_ref, bias1_ref, gain1_ref), (two_ref, bias2_ref, gain2_ref)):
        scaled = ref[0:1] * SCALE
        bias_ref[...] = scaled[:, 0:C]
        gain_ref[...] = pltpu.roll(scaled, 96, axis=1)[:, 0:C]
    cols = down(sum_ref[0:1])
    (mean, inv), _ = norms(stat_ref)
    b, g = cols[0:32] * (1.0 / CELLS), cols[32:64] * (1.0 / CELLS)
    amp = par_ref[0:32] * inv
    by = amp * inv * g
    off = amp * b - by * mean
    lane = lanes()
    sx, sy = mask_ref[0], mask_ref[1]
    inside_y = {0: jnp.where(sy > 0, 1.0, 0.0), B + 1: jnp.where(sy < 3, 1.0, 0.0)}

    def first(x, carry):
        gx = sx * B + x - 1
        inside_x = jnp.where((gx >= 0) & (gx < 4 * B), 1.0, 0.0)
        for y in range(B + 2):
            cut = slice(y * Z, (y + 1) * Z)
            value = amp * slope_ref[x, :, cut].astype(F32) - by * c1x_ref[x, :, cut].astype(F32) - off
            keep = inside_x * inside_y[y] if y in inside_y else inside_x
            grad[x, :, cut] = (value * keep).astype(BF16)
        return carry

    as_matrix(raw, w_ref)
    arriving[0].wait()
    lax.fori_loop(0, B + 2, first, 0)

    leaving = []
    for x in range(B):
        t = jnp.dot(w_ref[...], windows(grad, x, 2, 2, B), preferred_element_type=F32)
        rows = jnp.concatenate([unshift(t, y, lane)[None] for y in range(B)], 0)
        done[x] = jnp.swapaxes(rows, 0, 1).astype(BF16)
        leaving.append(pltpu.make_async_copy(done.at[x], out_ref.at[0, :, x], out_sems.at[x]))
        leaving[-1].start()
    for copy in leaving:
        copy.wait()


def filters_kernel(got_ref, one_ref, two_ref):
    rows = jnp.swapaxes(got_ref[...].astype(F32), 0, 1)
    for m, ref in enumerate((one_ref, two_ref)):
        for kz in range(3):
            for k in range(9):
                if k < 8:
                    slab, i = rows[m * 7 + kz * 2 + k // 4], k % 4
                else:
                    slab, i = rows[m * 7 + 6], kz
                ref[k // 3, k % 3, kz] = slab[:, i * C : (i + 1) * C]


def exchanged(array, axes):
    return lax.all_to_all(array, axes, 0, 0, tiled=True)


def per_device(
    volume, conv_one, conv_two, upper_grad, weight_one, weight_two, gain_one, bias_one, gain_two, bias_two
):
    pos = jnp.stack([lax.axis_index("sx"), lax.axis_index("sy")]).astype(jnp.int32)
    packed = jnp.concatenate([gain_one, bias_one, gain_two, bias_two])
    par = jnp.broadcast_to(packed[:, None], (128, 128))
    lanepar = jnp.broadcast_to(packed[None, :], (8, 128))
    everyone = shaped((256, 1, 128), F32)
    block = shaped((B, C, B * Z), BF16)
    three_fold = shaped((B, 3 * C, B * Z), BF16)
    near = shaped((B + 2, C, (B + 2) * Z), BF16)
    far = shaped((B + 4, C, (B + 4) * Z), BF16)
    near_wide, far_wide, block_wide = (shaped(a.shape, F32) for a in (near, far, block))
    row = shaped((8, 128), F32)

    def room(like):
        return pltpu.VMEM(like.shape, like.dtype)

    def sems(count):
        return pltpu.SemaphoreType.DMA((count,))

    along_x = shaped((len(layers_x(1)), C, B * Z), BF16)
    c1, c2, ug, vol3, send_down, send_up, stats = call(
        spread_kernel,
        [block, block, block, three_fold, along_x, along_x, everyone],
        scratch=[
            pltpu.VMEM((4, C, B, B, Z), BF16),
            room(three_fold),
            sems(4),
            sems(1),
        ],
        spaces=[HBM] * 4,
        homes=[VMEM] * 3 + [HBM] + [VMEM] * 3,
        limit=10,
    )(conv_one, conv_two, upper_grad, volume)
    up = [(i, i + 1) for i in range(3)]
    down_ = [(i + 1, i) for i in range(3)]
    x_low = lax.ppermute(send_up, "sx", up)
    x_high = lax.ppermute(send_down, "sx", down_)
    got_stats = exchanged(stats, ALL)
    along_y = shaped((len(slabs_y(1)), C, Z), BF16)
    send_down, send_up = call(pack_kernel, [along_y, along_y], spaces=[VMEM] * 5)(c1, c2, ug, x_low, x_high)
    y_low = lax.ppermute(send_up, "sy", up)
    y_high = lax.ppermute(send_down, "sy", down_)

    sums_two, stat_row, slope_two = call(
        sums_two_kernel, [everyone, row, block_wide], spaces=[VMEM] * 4
    )(got_stats, par, c2, ug)
    got_two = exchanged(sums_two, ALL)
    r_shape = shaped((128, 384), BF16)
    c1x, c2x, slopex, turn, act3, r = call(
        extend_kernel,
        [near, far, far_wide, near_wide, three_fold, r_shape],
        scratch=[
            room(r_shape), room(near), room(far), room(far_wide), room(near_wide), room(three_fold), room(far), room(three_fold), sems(11), sems(12)
        ],
        flops=5 * 10**9,
        spaces=[SMEM] + [VMEM] * 5 + [HBM] * 3,
        homes=[HBM] * 6,
        limit=16,
    )(pos, stat_row, par, c1, x_low, x_high, vol3, y_low, y_high)

    terms, slope, row_two = call(
        middle_kernel,
        [shaped((32, 24, 128), BF16), near, row],
        scratch=[
            pltpu.VMEM((3 * C, 9 * C), BF16), room(near), room(far), room(far_wide), room(near_wide), room(three_fold),
            room(three_fold), room(r_shape), room(far), sems(5), sems(8),
        ],
        flops=4 * 10**9,
        spaces=[SMEM] + [VMEM] * 6 + [HBM] * 7,
        limit=18,
    )(pos, got_two, stat_row, par, weight_two, c2, slope_two, c1x, c2x, slopex, turn, vol3, act3, r)

    got_terms = exchanged(terms, PLANE)
    relay = call(relay_kernel, shaped((8, 24, 128), BF16), spaces=[VMEM])(got_terms)
    got_relay = exchanged(relay, "dp_0")
    shares, row_one = call(
        share_kernel, [shaped((32, 16, 128), BF16), row], spaces=[VMEM] * 3
    )(got_relay, stat_row, lanepar)
    got_shares = exchanged(shares, PLANE)
    vector = shaped((1, C), F32)
    input_grad, gain_one_grad, bias_one_grad, gain_two_grad, bias_two_grad = call(
        last_kernel,
        [shaped((1, C, B, B, Z), BF16), vector, vector, vector, vector],
        scratch=[
            room(near), pltpu.VMEM((B, C, B, Z), BF16), pltpu.VMEM((3 * C, 9 * C), BF16), room(near), sems(8), sems(1)
        ],
        flops=4 * 10**9,
        spaces=[SMEM] + [VMEM] * 6 + [HBM],
        homes=[HBM] + [VMEM] * 4,
        limit=10,
    )(pos, row_one, row_two, stat_row, par, slope, weight_one, c1x)
    filters = shaped((3, 3, 3, C, C), F32)
    filter_one, filter_two = call(
        filters_kernel, [filters, filters], spaces=[VMEM]
    )(got_shares)
    return (
        input_grad, filter_one, filter_two, gain_one_grad[0], bias_one_grad[0], gain_two_grad[0], bias_two_grad[0]
    )


def solution(mesh):
    finer = Mesh(
        mesh.devices.reshape(8, 2, mesh.shape["sx"], mesh.shape["sy"]), ("dp_0", "dp_1", "sx", "sy")
    )
    field = P(DP, None, "sx", "sy", None)
    return jax.shard_map(
        per_device,
        mesh=finer,
        in_specs=(field,) * 4 + (P(),) * 6,
        out_specs=(field,) + (P(),) * 6,
        check_vma=False,
    )
```

```python
import math

import jax
import jax.numpy as jnp
from jax import lax
from jax.experimental import pallas as pl
from jax.experimental.pallas import tpu as pltpu
from jax.sharding import Mesh
from jax.sharding import PartitionSpec as P

DP = ("dp_0", "dp_1")
ALL = ("dp_0", "dp_1", "sx", "sy")
PLANE = ("dp_1", "sx", "sy")
EPS = 1e-05
F32 = jnp.float32
BF16 = jnp.bfloat16
C = 32
B = 8
Z = 128
CELLS = float(16 * 32 * 32 * Z)
SCALE = 1.0 / math.sqrt(CELLS)

VMEM = pltpu.MemorySpace.VMEM
SMEM = pltpu.MemorySpace.SMEM
HBM = pltpu.MemorySpace.HBM
FIELDS = (("c2", 2), ("ug", 2), ("c1", 1))


def span(side, width):
    return range(B - width, B) if side > 0 else range(width)


def landing(side, width):
    return range(B + width, B + 2 * width) if side > 0 else range(width)


def layers_x(side):
    return [(f, x) for f, w in FIELDS for x in span(side, w)]


def places_x(side):
    return [(f, x) for f, w in FIELDS for x in landing(side, w)]


def slabs_y(side):
    return [(f, y, x) for f, w in FIELDS for y in span(side, w) for x in range(B + 2 * w)]


def places_y(side):
    runs, first = [], 0
    for f, w in FIELDS:
        for y in landing(side, w):
            runs.append((first, B + 2 * w, f, y))
            first += B + 2 * w
    return runs


def call(kernel, outs, scratch=(), flops=0, spaces=(), limit=6, homes=None):
    single = not isinstance(outs, (list, tuple))
    shapes = [outs] if single else list(outs)
    homes = homes or [VMEM] * len(shapes)
    specs = [pl.BlockSpec(memory_space=space) for space in homes]
    shapes = [HBM(x.shape, x.dtype) if home == HBM else x for x, home in zip(shapes, homes)]
    f = pl.pallas_call(
        kernel,
        out_shape=shapes[0] if single else tuple(shapes),
        in_specs=[pl.BlockSpec(memory_space=space) for space in spaces],
        out_specs=specs[0] if single else tuple(specs),
        scratch_shapes=list(scratch),
        compiler_params=pltpu.CompilerParams(vmem_limit_bytes=limit * 2**20),
        cost_estimate=pl.CostEstimate(flops=flops, bytes_accessed=1 << 20, transcendentals=0),
    )

    def placed(*arguments):
        return f(
            *[
                pltpu.with_memory_space_constraint(x, HBM) if space == HBM else x
                for x, space in zip(arguments, spaces)
            ]
        )

    return placed


def started(pairs, sems):
    copies = [pltpu.make_async_copy(src, dst, sems.at[n]) for n, (src, dst) in enumerate(pairs)]
    for copy in copies:
        copy.start()
    return copies


def shaped(dims, kind):
    return jax.ShapeDtypeStruct(dims, kind)


def across(columns):
    return jnp.sum(jnp.transpose(columns), axis=0, keepdims=True)


def down(row):
    return jnp.transpose(jnp.broadcast_to(row, (128, 128)))


def arrived(ref):
    parts = [jnp.sum(ref[16 * n : 16 * n + 16], axis=0) for n in range(16)]
    while len(parts) > 1:
        parts = [a + b for a, b in zip(parts[::2], parts[1::2])]
    return parts[0]


def shifted(slab, lane):
    before = jnp.where(lane == 0, 0.0, pltpu.roll(slab, 1, axis=1))
    after = jnp.where(lane == Z - 1, 0.0, pltpu.roll(slab, Z - 1, axis=1))
    return jnp.concatenate([before, slab, after], 0)


def lanes():
    return lax.broadcasted_iota(jnp.int32, (C, Z), 1)


def spread_kernel(
    one_ref, two_ref, up_ref, vol_ref, c1_ref, c2_ref, ug_ref, vol3_out, down_ref, up_x_ref, stat_ref,
    held, vol3, sems, out_sem,
):
    sources = (("vol", vol_ref, None), ("c1", one_ref, c1_ref), ("c2", two_ref, c2_ref), ("ug", up_ref, ug_ref))
    half = [pl.ds(n * (B // 2), B // 2) for n in range(2)]
    halves = started([(vol_ref.at[0, :, cut], held.at[0, :, cut]) for cut in half], sems.at[pl.ds(3, 2)])
    copies = started([(src.at[0], held.at[n + 1]) for n, (_, src, _) in enumerate(sources[1:])], sems)
    lane = lanes()
    parts = []
    for n, (name, _, dst) in enumerate(sources):
        if n > 0:
            copies[n - 1].wait()
        total, squares = jnp.zeros((C, Z), F32), jnp.zeros((C, Z), F32)
        for x in range(B):
            if n == 0 and x % (B // 2) == 0:
                halves[x // (B // 2)].wait()
            turned_x = jnp.swapaxes(held[n, :, x].astype(F32), 0, 1)
            for y in range(B):
                slab = turned_x[y]
                if name == "vol":
                    vol3[x, :, y * Z : (y + 1) * Z] = shifted(slab, lane).astype(BF16)
                    continue
                if name in ("c1", "c2"):
                    total, squares = total + slab, squares + slab * slab
                dst[x, :, y * Z : (y + 1) * Z] = slab.astype(BF16)
        if name == "vol":
            leaving = pltpu.make_async_copy(vol3, vol3_out, out_sem.at[0])
            leaving.start()
        if name in ("c1", "c2"):
            parts += [total, squares]
    own = {"c1": c1_ref, "c2": c2_ref, "ug": ug_ref}
    for side, ref in ((-1, down_ref), (1, up_x_ref)):
        for i, (f, x) in enumerate(layers_x(side)):
            ref[i] = own[f][x]
    row = across(jnp.concatenate(parts, 0))
    stat_ref[...] = jnp.broadcast_to(row[None], stat_ref.shape)
    leaving.wait()


def pack_kernel(c1_ref, c2_ref, ug_ref, low_ref, high_ref, down_ref, up_ref):
    where = {}
    for f, w, ref in (("c1", 1, c1_ref), ("c2", 2, c2_ref), ("ug", 2, ug_ref)):
        for x in range(B):
            where[(f, x + w)] = (ref, x)
    for side, ref in ((-1, low_ref), (1, high_ref)):
        for i, key in enumerate(places_x(side)):
            where[key] = (ref, i)
    for side, out in ((-1, down_ref), (1, up_ref)):
        for i, (f, y, x) in enumerate(slabs_y(side)):
            ref, n = where[(f, x)]
            out[i] = ref[n, :, y * Z : (y + 1) * Z]


def extend_kernel(
    pos_ref, stat_ref, par_ref, c1_ref, xlow_ref, xhigh_ref, vol3_in, ylow_in, yhigh_in,
    c1x_out, c2x_out, slopex_out, turn_out, act3_out, r_out, r_ref, c1x, c2x, slopex, turn, act3, ugx, vol3, sems, out_sems,
):
    target = {"c1": c1x, "c2": c2x, "ug": ugx}
    pairs = []
    for side, ref in ((-1, ylow_in), (1, yhigh_in)):
        for first, count, f, y in places_y(side):
            pairs.append((ref.at[pl.ds(first, count)], target[f].at[:, :, pl.ds(y * Z, Z)]))
    pairs.append((vol3_in, vol3))
    arriving = started(pairs, sems)
    (mean1, inv1), (mean2, inv2) = norms(stat_ref)
    gain1, bias1, gain2, bias2 = par_ref[0:32], par_ref[32:64], par_ref[64:96], par_ref[96:128]
    lane = lanes()

    def activation(x, carry):
        for y in range(B):
            cut = slice(y * Z, (y + 1) * Z)
            cent = (c1_ref[x, :, cut].astype(F32) - mean1) * inv1
            pre = gain1 * cent + bias1
            s = sigmoid(pre)
            act3[x, :, cut] = shifted((pre * s).astype(BF16).astype(F32), lane).astype(BF16)
            turn[x + 1, :, (y + 1) * Z : (y + 2) * Z] = s * (1.0 + pre * (1.0 - s))
        return carry

    lax.fori_loop(0, B, activation, 0)
    leaving = started([(act3, act3_out)], out_sems)
    for x in range(B):
        c1x[x + 1, :, Z : (1 + B) * Z] = c1_ref[x]
    width = dict(FIELDS)
    for side, ref in ((-1, xlow_ref), (1, xhigh_ref)):
        for i, (f, x) in enumerate(places_x(side)):
            w = width[f]
            target[f][x, :, w * Z : (w + B) * Z] = ref[i]
    for copy in arriving[:-1]:
        copy.wait()
    leaving += started([(c1x, c1x_out)] + [(c2x.at[cut], c2x_out.at[cut]) for cut in RIM], out_sems.at[pl.ds(1, 5)])

    def slope_at(x, y):
        cut = slice(y * Z, (y + 1) * Z)
        cent = (c2x[x, :, cut].astype(F32) - mean2) * inv2
        slopex[x, :, cut] = ugx[x, :, cut].astype(F32) * silu_slope(gain2 * cent + bias2)

    def ends(i, carry):
        x = jnp.where(i < 2, i, i + B)
        for y in range(B + 4):
            slope_at(x, y)
        return carry

    lax.fori_loop(0, 4, ends, 0)

    def between(x, carry):
        for y in (0, 1, B + 2, B + 3):
            slope_at(x + 2, y)
        return carry

    lax.fori_loop(0, B, between, 0)
    leaving += started([(slopex.at[cut], slopex_out.at[cut]) for cut in RIM], out_sems.at[pl.ds(6, 4)])

    def turn_at(x, y):
        cut = slice(y * Z, (y + 1) * Z)
        cent = (c1x[x, :, cut].astype(F32) - mean1) * inv1
        turn[x, :, cut] = silu_slope(gain1 * cent + bias1)

    for x in (0, B + 1):
        for y in range(B + 2):
            turn_at(x, y)

    def sides(x, carry):
        turn_at(x + 1, 0)
        turn_at(x + 1, B + 1)
        return carry

    lax.fori_loop(0, B, sides, 0)
    leaving += started([(turn, turn_out)], out_sems.at[pl.ds(10, 1)])

    sx, sy = pos_ref[0], pos_ref[1]
    row = lax.broadcasted_iota(jnp.int32, (16, B * Z), 0)
    gy = sy * B + lax.broadcasted_iota(jnp.int32, (16, B * Z), 1) // Z
    wy = gy + 1 - row % 3
    ok_y = (wy >= 0) & (wy < 4 * B) & (row < 9)

    def body(x, acc):
        wx = sx * B + x + 1 - row // 3
        inside = jnp.where(ok_y & (wx >= 0) & (wx < 4 * B), 1.0, 0.0).astype(BF16)
        lhs = jnp.concatenate([windows(c1x, x, 2, 2, B), inside], 0)
        return acc + lax.dot_general(lhs, vol3[x], TRANSPOSED, preferred_element_type=F32)

    arriving[-1].wait()
    acc = lax.fori_loop(0, B, body, jnp.zeros((9 * C + 16, 3 * C), F32), unroll=2)
    r_ref[...] = turned(acc).astype(BF16)
    leaving += started([(r_ref, r_out)], out_sems.at[pl.ds(11, 1)])
    for copy in leaving:
        copy.wait()


RIM = (
    (pl.ds(0, 2),),
    (pl.ds(B + 2, 2),),
    (pl.ds(2, B), slice(None), pl.ds(0, 2 * Z)),
    (pl.ds(2, B), slice(None), pl.ds((B + 2) * Z, 2 * Z)),
)

TRANSPOSED = (((1,), (1,)), ((), ()))


def turned(acc):
    rows = acc.shape[0]
    full = jnp.concatenate([acc, jnp.zeros((384 - rows, 3 * C), F32)], 0)
    full = jnp.concatenate([full, jnp.zeros((384, 128 - 3 * C), F32)], 1)
    return jnp.concatenate([jnp.transpose(full[i * 128 : (i + 1) * 128]) for i in range(3)], 1)


def moments(total, squares):
    mean = total * (1.0 / CELLS)
    inv = lax.rsqrt(squares * (1.0 / CELLS) - mean * mean + EPS)
    return mean, inv


def norms(stat_ref):
    cols = down(stat_ref[0:1])
    return moments(cols[0:32], cols[32:64]), moments(cols[64:96], cols[96:128])


def sigmoid(v):
    return 0.5 * jnp.tanh(0.5 * v) + 0.5


def silu_slope(v):
    s = sigmoid(v)
    return s * (1.0 + v * (1.0 - s))


def sums_two_kernel(got_ref, par_ref, c2_ref, ug_ref, out_ref, row_ref, slope_ref):
    row = arrived(got_ref)
    row_ref[...] = jnp.broadcast_to(row, (8, 128))
    _, (mean2, inv2) = norms(row_ref)
    gain, bias = par_ref[64:96], par_ref[96:128]

    def body(x, acc):
        b, g = acc
        for y in range(B):
            cent = (c2_ref[x, :, y * Z : (y + 1) * Z].astype(F32) - mean2) * inv2
            up = ug_ref[x, :, y * Z : (y + 1) * Z].astype(F32)
            slope = up * silu_slope(gain * cent + bias)
            slope_ref[x, :, y * Z : (y + 1) * Z] = slope
            b, g = b + slope, g + slope * cent
        return b, g

    zero = jnp.zeros((C, Z), F32)
    b, g = lax.fori_loop(0, B, body, (zero, zero), unroll=4)
    out = across(jnp.concatenate([b, g, zero, zero], 0))
    out_ref[...] = jnp.broadcast_to(out[None], out_ref.shape)


def windows(ref, x, first, y_first, count):
    parts = []
    for kx in range(3):
        for ky in range(3):
            parts.append(ref[x + first - kx, :, (y_first - ky) * Z : (y_first - ky + count) * Z])
    return jnp.concatenate(parts, 0)


def unshift(t, y, lane):
    left = t[0:C, y * Z : (y + 1) * Z]
    mid = t[C : 2 * C, y * Z : (y + 1) * Z]
    right = t[2 * C : 3 * C, y * Z : (y + 1) * Z]
    out = mid + jnp.where(lane == Z - 1, 0.0, pltpu.roll(left, Z - 1, axis=1))
    return out + jnp.where(lane == 0, 0.0, pltpu.roll(right, 1, axis=1))


def as_matrix(src, dst):
    for kz in range(3):
        parts = [src[kx, ky, kz].astype(F32) for kx in range(3) for ky in range(3)]
        dst[kz * C : (kz + 1) * C, :] = jnp.concatenate(parts, 1).astype(BF16)


def three(value):
    hi = value.astype(BF16).astype(F32)
    mid = (value - hi).astype(BF16).astype(F32)
    lo = value - hi - mid
    return hi, mid, lo


MARKS = 96


def moved(row, lanes_up):
    return pltpu.roll(row, lanes_up, axis=1) if lanes_up else row


def sum_rows(sums):
    lane = lax.broadcasted_iota(jnp.int32, (1, 128), 1)
    hi, mid, lo = (jnp.where(lane < 64, part, 0.0) for part in three(sums))
    return hi + moved(mid, 64), lo


def sums_of(total):
    return total[21:22] + moved(total[21:22], 64) + total[22:23]


def middle_kernel(
    pos_ref, got_ref, stat_ref, par_ref, raw, c2_ref, slope_two_ref, c1x_in, c2x_in, slopex_in, turn_in, vol3_in, act3_in, r_in,
    msg_ref, slope_ref, row_ref, w_ref, c1x_ref, c2x_ref, slopex_ref, turn_ref, vol3_ref, act3_ref, r_ref,
    grad, sems, row_sems,
):
    early = started(
        [(src.at[cut], dst.at[cut]) for cut in RIM for src, dst in ((slopex_in, slopex_ref), (c2x_in, c2x_ref))],
        row_sems,
    )
    arriving = started(
        [
            (turn_in, turn_ref),
            (c1x_in, c1x_ref),
            (vol3_in, vol3_ref),
            (act3_in, act3_ref),
            (r_in, r_ref),
        ],
        sems,
    )
    sx, sy = pos_ref[0], pos_ref[1]
    row = arrived(got_ref)
    row_ref[...] = jnp.broadcast_to(row, (8, 128))
    cols = down(row)
    (mean1, inv1), (mean2, inv2) = norms(stat_ref)
    amp = par_ref[64:96] * inv2
    by = amp * inv2 * cols[32:64] * (1.0 / CELLS)
    off = amp * cols[0:32] * (1.0 / CELLS) - by * mean2
    lane = lanes()
    inside_y = {
        y: jnp.where(sy > 0, 1.0, 0.0) if y < 2 else jnp.where(sy < 3, 1.0, 0.0)
        for y in (0, 1, B + 2, B + 3)
    }

    def own(x, carry):
        for y in range(B):
            cut = slice(y * Z, (y + 1) * Z)
            value = amp * slope_two_ref[x, :, cut] - by * c2_ref[x, :, cut].astype(F32) - off
            grad[x + 2, :, (y + 2) * Z : (y + 3) * Z] = value.astype(BF16)
        return carry

    lax.fori_loop(0, B, own, 0, unroll=2)
    as_matrix(raw, w_ref)

    def rim_at(x, y, inside_x):
        cut = slice(y * Z, (y + 1) * Z)
        value = amp * slopex_ref[x, :, cut] - by * c2x_ref[x, :, cut].astype(F32) - off
        keep = inside_x * inside_y[y] if y in inside_y else inside_x
        grad[x, :, cut] = (value * keep).astype(BF16)

    for copy in early[:4]:
        copy.wait()

    def ends(i, carry):
        x = jnp.where(i < 2, i, i + B)
        gx = sx * B + x - 2
        inside_x = jnp.where((gx >= 0) & (gx < 4 * B), 1.0, 0.0)
        for y in range(B + 4):
            rim_at(x, y, inside_x)
        return carry

    lax.fori_loop(0, 4, ends, 0)
    for copy in early[4:]:
        copy.wait()

    def sides(x, carry):
        for y in (0, 1, B + 2, B + 3):
            rim_at(x + 2, y, 1.0)
        return carry

    lax.fori_loop(0, B, sides, 0)
    arriving[0].wait()
    arriving[1].wait()
    inside_y = {0: jnp.where(sy > 0, 1.0, 0.0), B + 1: jnp.where(sy < 3, 1.0, 0.0)}

    def second(x, acc):
        b, g = acc
        gx = sx * B + x - 1
        inside_x = jnp.where((gx >= 0) & (gx < 4 * B), 1.0, 0.0)
        own_x = jnp.where((x >= 1) & (x <= B), 1.0, 0.0)
        t = jnp.dot(w_ref[...], windows(grad, x, 2, 2, B + 2), preferred_element_type=F32)
        bx, gsum = jnp.zeros((C, Z), F32), jnp.zeros((C, Z), F32)
        for y in range(B + 2):
            cut = slice(y * Z, (y + 1) * Z)
            slope = unshift(t, y, lane) * turn_ref[x, :, cut]
            if 1 <= y <= B:
                bx, gsum = bx + slope, gsum + slope * c1x_ref[x, :, cut].astype(F32)
            inside = inside_x * inside_y[y] if y in inside_y else inside_x
            slope_ref[x, :, cut] = (slope * inside).astype(BF16)
        gsum = (gsum - mean1 * bx) * inv1
        return b + bx * own_x, g + gsum * own_x

    zero = jnp.zeros((C, Z), F32)
    b, g = lax.fori_loop(0, B + 2, second, (zero, zero), unroll=5)

    def third(x, acc):
        s, f = acc
        s = s + lax.dot_general(windows(slope_ref, x, 2, 2, B), vol3_ref[x], TRANSPOSED, preferred_element_type=F32)
        f = f + lax.dot_general(windows(grad, x, 3, 3, B), act3_ref[x], TRANSPOSED, preferred_element_type=F32)
        return s, f

    for copy in arriving[2:]:
        copy.wait()
    empty = jnp.zeros((9 * C, 3 * C), F32)
    s, f = lax.fori_loop(0, B, third, (empty, empty), unroll=4)
    sums = across(jnp.concatenate([b, g, zero, zero], 0))
    rows = []
    for marked, part in ((False, turned(s)), (True, r_ref[...].astype(F32)), (False, turned(f))):
        packed = zero
        for kz in range(3):
            band = part[kz * C : (kz + 1) * C]
            rows += [band[:, 0:128][None], band[:, 128:256][None]]
            end = band[:, 256:384]
            packed += moved(jnp.where(lane < C, end, 0.0), kz * C)
            if marked:
                packed += moved(jnp.where((lane >= C) & (lane < C + 9), end, 0.0), MARKS - C + 9 * kz)
        rows.append(packed[None])
    rows += [jnp.broadcast_to(part, (C, 128))[None] for part in sum_rows(sums)] + [zero[None]]
    for n in range(3):
        block = jnp.swapaxes(jnp.concatenate(rows[8 * n : 8 * n + 8], 0), 0, 1)
        msg_ref[:, 8 * n : 8 * n + 8, :] = block.astype(BF16)


def relay_kernel(got_ref, out_ref):
    total = jnp.sum(got_ref[...].astype(F32), axis=0)
    first, second = sum_rows(sums_of(total))
    out = jnp.concatenate([total[0:21], first, second, total[23:24]], 0).astype(BF16)
    out_ref[...] = jnp.broadcast_to(out[None], out_ref.shape)


def selected(rows, choice):
    parts = jnp.concatenate(three(rows), 0).astype(BF16)
    out = jnp.dot(parts, choice.astype(BF16), preferred_element_type=F32)
    return out[0:8] + out[8:16] + out[16:24]


def share_kernel(got_ref, stat_ref, lanepar_ref, out_ref, row_ref):
    total = jnp.sum(got_ref[...].astype(F32), axis=0)
    sums = sums_of(total)
    row_ref[...] = jnp.broadcast_to(sums, (8, 128))
    lane = lax.broadcasted_iota(jnp.int32, (1, 128), 1)
    stat = stat_ref[0:1]
    mean = stat * (1.0 / CELLS)
    squares = pltpu.roll(stat, 96, axis=1) * (1.0 / CELLS)
    inv = lax.rsqrt(jnp.where(lane < C, squares - mean * mean, 0.0) + EPS)
    g = pltpu.roll(sums, 96, axis=1)
    alpha = lanepar_ref[0:1] * inv
    gamma = alpha * inv * g * (1.0 / CELLS)
    delta = alpha * sums * (1.0 / CELLS) - gamma * mean
    rows = jnp.where(lane < C, jnp.concatenate([alpha, gamma, delta], 0), 0.0)
    rows = jnp.concatenate([rows, jnp.zeros((5, 128), F32)], 0)
    a = lax.broadcasted_iota(jnp.int32, (128, 896), 0)
    o = lax.broadcasted_iota(jnp.int32, (128, 896), 1)
    tile = jnp.where(o[:, 0:128] % C == a[:, 0:128], 1.0, 0.0)
    wide = selected(rows, tile)
    row = o // 128
    block = (o % 128) // C
    mark = jnp.where(row < 6, MARKS + 9 * (row // 2) + 4 * (row % 2) + block, MARKS + 9 * block + 8)
    spread = jnp.where((mark == a) & ((row < 6) | (block < 3)), 1.0, 0.0)
    marks = jnp.concatenate([total[13:14], jnp.zeros((7, 128), F32)], 0)
    ones = selected(marks, spread)
    parts = []
    for r in range(7):
        parts.append(
            wide[0:1] * total[r : r + 1]
            - wide[1:2] * total[7 + r : 8 + r]
            - wide[2:3] * ones[0:1, r * 128 : (r + 1) * 128]
        )
    out = jnp.concatenate(parts + [total[14:21], jnp.zeros((2, 128), F32)], 0) * SCALE
    out_ref[...] = jnp.broadcast_to(out.astype(BF16)[None], out_ref.shape)


def last_kernel(
    mask_ref, sum_ref, two_ref, stat_ref, par_ref, slope_ref, raw, c1x_in,
    out_ref, gain1_ref, bias1_ref, gain2_ref, bias2_ref, grad, done, w_ref, c1x_ref, out_sems, sems,
):
    arriving = started([(c1x_in, c1x_ref)], sems)
    for ref, bias_ref, gain_ref in ((sum_ref, bias1_ref, gain1_ref), (two_ref, bias2_ref, gain2_ref)):
        scaled = ref[0:1] * SCALE
        bias_ref[...] = scaled[:, 0:C]
        gain_ref[...] = pltpu.roll(scaled, 96, axis=1)[:, 0:C]
    cols = down(sum_ref[0:1])
    (mean, inv), _ = norms(stat_ref)
    b, g = cols[0:32] * (1.0 / CELLS), cols[32:64] * (1.0 / CELLS)
    amp = par_ref[0:32] * inv
    by = amp * inv * g
    off = amp * b - by * mean
    lane = lanes()
    sx, sy = mask_ref[0], mask_ref[1]
    inside_y = {0: jnp.where(sy > 0, 1.0, 0.0), B + 1: jnp.where(sy < 3, 1.0, 0.0)}

    def first(x, carry):
        gx = sx * B + x - 1
        inside_x = jnp.where((gx >= 0) & (gx < 4 * B), 1.0, 0.0)
        for y in range(B + 2):
            cut = slice(y * Z, (y + 1) * Z)
            value = amp * slope_ref[x, :, cut].astype(F32) - by * c1x_ref[x, :, cut].astype(F32) - off
            keep = inside_x * inside_y[y] if y in inside_y else inside_x
            grad[x, :, cut] = (value * keep).astype(BF16)
        return carry

    as_matrix(raw, w_ref)
    arriving[0].wait()
    lax.fori_loop(0, B + 2, first, 0)

    leaving = []
    for x in range(B):
        t = jnp.dot(w_ref[...], windows(grad, x, 2, 2, B), preferred_element_type=F32)
        rows = jnp.concatenate([unshift(t, y, lane)[None] for y in range(B)], 0)
        done[x] = jnp.swapaxes(rows, 0, 1).astype(BF16)
        leaving.append(pltpu.make_async_copy(done.at[x], out_ref.at[0, :, x], out_sems.at[x]))
        leaving[-1].start()
    for copy in leaving:
        copy.wait()


def filters_kernel(got_ref, one_ref, two_ref):
    rows = jnp.swapaxes(got_ref[...].astype(F32), 0, 1)
    for m, ref in enumerate((one_ref, two_ref)):
        for kz in range(3):
            for k in range(9):
                if k < 8:
                    slab, i = rows[m * 7 + kz * 2 + k // 4], k % 4
                else:
                    slab, i = rows[m * 7 + 6], kz
                ref[k // 3, k % 3, kz] = slab[:, i * C : (i + 1) * C]


def exchanged(array, axes):
    return lax.all_to_all(array, axes, 0, 0, tiled=True)


def per_device(
    volume, conv_one, conv_two, upper_grad, weight_one, weight_two, gain_one, bias_one, gain_two, bias_two
):
    pos = jnp.stack([lax.axis_index("sx"), lax.axis_index("sy")]).astype(jnp.int32)
    packed = jnp.concatenate([gain_one, bias_one, gain_two, bias_two])
    par = jnp.broadcast_to(packed[:, None], (128, 128))
    lanepar = jnp.broadcast_to(packed[None, :], (8, 128))
    everyone = shaped((256, 1, 128), F32)
    block = shaped((B, C, B * Z), BF16)
    three_fold = shaped((B, 3 * C, B * Z), BF16)
    near = shaped((B + 2, C, (B + 2) * Z), BF16)
    far = shaped((B + 4, C, (B + 4) * Z), BF16)
    near_wide, far_wide, block_wide = (shaped(a.shape, F32) for a in (near, far, block))
    row = shaped((8, 128), F32)

    def room(like):
        return pltpu.VMEM(like.shape, like.dtype)

    def sems(count):
        return pltpu.SemaphoreType.DMA((count,))

    along_x = shaped((len(layers_x(1)), C, B * Z), BF16)
    c1, c2, ug, vol3, send_down, send_up, stats = call(
        spread_kernel,
        [block, block, block, three_fold, along_x, along_x, everyone],
        scratch=[
            pltpu.VMEM((4, C, B, B, Z), BF16),
            room(three_fold),
            sems(5),
            sems(1),
        ],
        spaces=[HBM] * 4,
        homes=[VMEM] * 3 + [HBM] + [VMEM] * 3,
        limit=10,
    )(conv_one, conv_two, upper_grad, volume)
    up = [(i, i + 1) for i in range(3)]
    down_ = [(i + 1, i) for i in range(3)]
    x_low = lax.ppermute(send_up, "sx", up)
    x_high = lax.ppermute(send_down, "sx", down_)
    got_stats = exchanged(stats, ALL)
    along_y = shaped((len(slabs_y(1)), C, Z), BF16)
    send_down, send_up = call(pack_kernel, [along_y, along_y], spaces=[VMEM] * 5)(c1, c2, ug, x_low, x_high)
    y_low = lax.ppermute(send_up, "sy", up)
    y_high = lax.ppermute(send_down, "sy", down_)

    sums_two, stat_row, slope_two = call(
        sums_two_kernel, [everyone, row, block_wide], spaces=[VMEM] * 4
    )(got_stats, par, c2, ug)
    got_two = exchanged(sums_two, ALL)
    r_shape = shaped((128, 384), BF16)
    c1x, c2x, slopex, turn, act3, r = call(
        extend_kernel,
        [near, far, far_wide, near_wide, three_fold, r_shape],
        scratch=[
            room(r_shape), room(near), room(far), room(far_wide), room(near_wide), room(three_fold), room(far), room(three_fold), sems(11), sems(12)
        ],
        flops=5 * 10**9,
        spaces=[SMEM] + [VMEM] * 5 + [HBM] * 3,
        homes=[HBM] * 6,
        limit=16,
    )(pos, stat_row, par, c1, x_low, x_high, vol3, y_low, y_high)

    terms, slope, row_two = call(
        middle_kernel,
        [shaped((32, 24, 128), BF16), near, row],
        scratch=[
            pltpu.VMEM((3 * C, 9 * C), BF16), room(near), room(far), room(far_wide), room(near_wide), room(three_fold),
            room(three_fold), room(r_shape), room(far), sems(5), sems(8),
        ],
        flops=4 * 10**9,
        spaces=[SMEM] + [VMEM] * 6 + [HBM] * 7,
        limit=18,
    )(pos, got_two, stat_row, par, weight_two, c2, slope_two, c1x, c2x, slopex, turn, vol3, act3, r)

    got_terms = exchanged(terms, PLANE)
    relay = call(relay_kernel, shaped((8, 24, 128), BF16), spaces=[VMEM])(got_terms)
    got_relay = exchanged(relay, "dp_0")
    shares, row_one = call(
        share_kernel, [shaped((32, 16, 128), BF16), row], spaces=[VMEM] * 3
    )(got_relay, stat_row, lanepar)
    got_shares = exchanged(shares, PLANE)
    vector = shaped((1, C), F32)
    input_grad, gain_one_grad, bias_one_grad, gain_two_grad, bias_two_grad = call(
        last_kernel,
        [shaped((1, C, B, B, Z), BF16), vector, vector, vector, vector],
        scratch=[
            room(near), pltpu.VMEM((B, C, B, Z), BF16), pltpu.VMEM((3 * C, 9 * C), BF16), room(near), sems(8), sems(1)
        ],
        flops=4 * 10**9,
        spaces=[SMEM] + [VMEM] * 6 + [HBM],
        homes=[HBM] + [VMEM] * 4,
        limit=10,
    )(pos, row_one, row_two, stat_row, par, slope, weight_one, c1x)
    filters = shaped((3, 3, 3, C, C), F32)
    filter_one, filter_two = call(
        filters_kernel, [filters, filters], spaces=[VMEM]
    )(got_shares)
    return (
        input_grad, filter_one, filter_two, gain_one_grad[0], bias_one_grad[0], gain_two_grad[0], bias_two_grad[0]
    )


def solution(mesh):
    finer = Mesh(
        mesh.devices.reshape(8, 2, mesh.shape["sx"], mesh.shape["sy"]), ("dp_0", "dp_1", "sx", "sy")
    )
    field = P(DP, None, "sx", "sy", None)
    return jax.shard_map(
        per_device,
        mesh=finer,
        in_specs=(field,) * 4 + (P(),) * 6,
        out_specs=(field,) + (P(),) * 6,
        check_vma=False,
    )
```
